256 devices in a mesh: rep: 1, dp: 256 (over x, y, z, core).
Axes of the slice: x: 4, y: 4, z: 8, core: 2. Of those that a mesh axis runs over, the one named last changes fastest.
Arguments:
- x: bfloat16 [256, 1024, 1536], P(('rep', 'dp'))
- dy: bfloat16 [256, 1024, 1536], P(('rep', 'dp'))
- w_gate: bfloat16 [2, 1536, 3584], replicated
- w_up: bfloat16 [2, 1536, 3584], replicated
- w_down: bfloat16 [2, 3584, 1536], replicated
- m_w_gate: float32 [2, 1536, 3584], P(None, 'dp')
- m_w_up: float32 [2, 1536, 3584], P(None, 'dp')
- m_w_down: float32 [2, 3584, 1536], P(None, 'dp')
- v_w_gate: float32 [2, 1536, 3584], P(None, 'dp')
- v_w_up: float32 [2, 1536, 3584], P(None, 'dp')
- v_w_down: float32 [2, 3584, 1536], P(None, 'dp')
Outputs:
- output 1: bfloat16 [2, 1536, 3584], P('rep')
- output 2: bfloat16 [2, 1536, 3584], P('rep')
- output 3: bfloat16 [2, 3584, 1536], P('rep')
- output 4: float32 [2, 1536, 3584], P('rep', 'dp')
- output 5: float32 [2, 1536, 3584], P('rep', 'dp')
- output 6: float32 [2, 3584, 1536], P('rep', 'dp')
- output 7: float32 [2, 1536, 3584], P('rep', 'dp')
- output 8: float32 [2, 1536, 3584], P('rep', 'dp')
- output 9: float32 [2, 3584, 1536], P('rep', 'dp')
All inputs are finite; a program needn't handle non-finite values.
Results may differ from the reference program's by a relative error of at most 0.022.
Values are sent between devices in bfloat16 or wider.
A program may use at most 768 MiB of HBM per device.

```python
import jax
import jax.numpy as jnp
from jax import lax

SEQUENCES = 256
TOKENS = 1024
D = 1536
FF = 3584
LAYERS = 2
NAMES = ("w_gate", "w_up", "w_down")
SHAPES = {"w_gate": (LAYERS, D, FF), "w_up": (LAYERS, D, FF), "w_down": (LAYERS, FF, D)}


def bump(key, n, height):
    away = (jnp.arange(n, dtype=jnp.int32) - jax.random.randint(key, (), 0, n, jnp.int32)) % n
    return jnp.where(away < n // 8, height, 1.0)


def together(key, own, strength):
    shared = jax.random.normal(key, own.shape[1:], jnp.float32)
    return (own + strength * shared) * lax.rsqrt(1 + strength * strength)


def setup_inputs(seed: int = 0, part: int = 0) -> dict:
    kx, kdy, ka, kb, kz, kf, kh, kl, *keys = jax.random.split(jax.random.key(seed), 8 + 3 * len(NAMES))
    kx, kdy, ka, kb = (jax.random.fold_in(k, part) for k in (kx, kdy, ka, kb))
    kw, km, kv = (keys[i::3] for i in range(3))
    shape = (SEQUENCES, TOKENS, D)
    much_x, much_dy = jax.random.uniform(kz, (2,), jnp.float32, 0.0, 1.0)
    loud = 2.0 ** jax.random.uniform(jax.random.fold_in(kz, 1), (), jnp.float32, -1.0, 2.0)
    layers = 2.0 ** jax.random.uniform(kl, (LAYERS, 1, 1), jnp.float32, -1.0, 1.0)
    x = together(ka, jax.random.normal(kx, shape, jnp.float32), much_x) * bump(kf, D, 4.0)
    dy = together(kb, jax.random.normal(kdy, shape, jnp.float32), much_dy)
    drawn = {"x": x.astype(jnp.bfloat16), "dy": (loud * dy * (SEQUENCES * TOKENS) ** -0.5).astype(jnp.bfloat16)}
    for key, name in zip(kw, NAMES, strict=True):
        w = jax.random.normal(key, SHAPES[name], jnp.float32) * SHAPES[name][1] ** -0.5
        drawn[name] = (w * {"w_gate": 1.0, "w_up": bump(kh, FF, 4.0), "w_down": layers}[name]).astype(jnp.bfloat16)
    for key, name in zip(km, NAMES, strict=True):
        drawn[f"m_{name}"] = 0.1 * jax.random.normal(key, SHAPES[name], jnp.float32)
    for key, name in zip(kv, NAMES, strict=True):
        drawn[f"v_{name}"] = jax.random.uniform(key, SHAPES[name], jnp.float32, 0.005, 0.015)
    return drawn


def matmul(a, w):
    return jnp.dot(a, w, preferred_element_type=jnp.float32).astype(jnp.bfloat16)


def normed(h):
    wide = h.astype(jnp.float32)
    scale = lax.rsqrt(jnp.mean(wide**2, -1, keepdims=True) + 1e-6)
    return (wide * scale).astype(jnp.bfloat16)


def layer(h, w):
    a = normed(h)
    gate = jnp.dot(a, w["w_gate"], preferred_element_type=jnp.float32)
    up = jnp.dot(a, w["w_up"], preferred_element_type=jnp.float32)
    return h + matmul((jax.nn.silu(gate) * up).astype(jnp.bfloat16), w["w_down"])


def adamw(w, m, v, g):
    m = 0.9 * m + 0.1 * g
    v = 0.95 * v + 0.05 * g * g
    step = m * lax.rsqrt(v + 1e-8) + 0.1 * w
    return (w - 0.02 * step).astype(jnp.bfloat16), m, v


def clipped(gradients, sum_of_squares, count):
    factor = jnp.minimum(1.0, 0.5 * lax.rsqrt(sum_of_squares / count + 1e-30))
    return [g * factor for g in gradients]


def stack(weights, h):
    return lax.scan(lambda h, w: (layer(h, w), None), h, weights)[0]


def reference(x, dy, w_gate, w_up, w_down, m_w_gate, m_w_up, m_w_down, v_w_gate, v_w_up, v_w_down):
    weights = dict(zip(NAMES, (w_gate, w_up, w_down), strict=True))

    def take(so_far, sequence):
        h, by_y = sequence
        _, back = jax.vjp(lambda w: stack(w, h), weights)
        return jax.tree.map(lambda total, term: total + term.astype(jnp.float32), so_far, back(by_y)[0]), None

    none_yet = {name: jnp.zeros(w.shape, jnp.float32) for name, w in weights.items()}
    by_weights, _ = lax.scan(take, none_yet, (x, dy))
    gradients = [by_weights[name].astype(jnp.bfloat16).astype(jnp.float32) for name in NAMES]
    gradients = clipped(gradients, sum(jnp.sum(g * g) for g in gradients), sum(g.size for g in gradients))
    new = [
        adamw(w.astype(jnp.float32), m, v, g)
        for w, m, v, g in zip((w_gate, w_up, w_down), (m_w_gate, m_w_up, m_w_down), (v_w_gate, v_w_up, v_w_down), gradients, strict=True)
    ]
    return tuple(one[which] for which in range(3) for one in new)
```

```python
import functools
import jax, jax.numpy as jnp
from jax import lax
from jax.experimental import pallas as pl
from jax.experimental.pallas import tpu as pltpu

bf16, f32 = jnp.bfloat16, jnp.float32
MATS = 6
UNIT = (24, 896)
DOWN = (56, 384)
TILE = (8, 128)
PADS = (8, 16)
ORDERS = ("xyz", "yzx", "zxy")
COLUMNS = ((0, 384), (384, 256), (640, 256))
KINDS = ("s", "f", "z", "d", "e")
SCATTER_TIMES, SCATTER_STEP = "#:LMWbb{'6CCMMXaajjs#/'85CTT]ghq", 18
GATHER_TIMES, GATHER_STEPS = '#-.4799Yj~#337;<DEOPQ_oi#((3@AAKX\\bgoy', (4, 14)
MESH = pl.DeviceIdType.MESH
START, MORE = 0, 1
NORTH, SOUTH = 0, 1


def time_of(character):
    return ord(character) - ord("#")


class Torus:
    def __init__(self, dims):
        self.dims = dict(zip("xyz", dims))
        self.cores = 2
        _, Y, Z = dims
        self.stride = dict(zip("xyz", (Y * Z * self.cores, Z * self.cores, self.cores)))
        self.rep, self.idx = lax.axis_index("rep"), lax.axis_index("dp")
        self.at = {d: lax.rem(lax.div(self.idx, self.stride[d]), self.dims[d]) for d in "xyz"}
        self.core = lax.rem(self.idx, self.cores)

    def wrap(self, d, value):
        n = self.dims[d]
        return lax.rem(value + n, n)

    def beside(self, d, offset):
        return (self.rep, self.idx + (self.wrap(d, self.at[d] + offset) - self.at[d]) * self.stride[d])

    def partner(self):
        return (self.rep, self.idx + 1 - 2 * self.core)

    def everyone(self):
        return [self.beside(d, o) for d in "xyz" for o in range(1, self.dims[d])]

    def group(self, s):
        return (self.rep, self.idx - lax.rem(self.idx, 4) + s)

    def enter(self):
        me = lax.rem(self.idx, 4)
        barrier = pltpu.get_barrier_semaphore()
        devices = self.everyone() + [self.partner(), self.group(lax.rem(me + 3 - 2 * self.core, 4))]
        for device in devices:
            signal(barrier, device)
        pl.semaphore_wait(barrier, len(devices))


def signal(sem, device):
    pl.semaphore_signal(sem, inc=1, device_id=device, device_id_type=MESH)


def remote(src, dst, send, recv, device):
    return pltpu.make_async_remote_copy(src_ref=src, dst_ref=dst, send_sem=send, recv_sem=recv, device_id=device, device_id_type=MESH)


class Ring:
    def __init__(self, color, phase, d, n):
        self.name = f"{color.k}{phase}"
        self.color, self.phase, self.d, self.n = color, phase, d, n
        self.steps = (n // 2, (n - 1) // 2)
        self.sides = [side for side in (NORTH, SOUTH) if self.steps[side]]

    def message(self, side, m):
        return m + side * self.steps[NORTH]


class Color:
    def __init__(self, k, dims):
        self.k, self.order = k, ORDERS[k]
        start, self.width = COLUMNS[k]
        self.columns = pl.ds(start, self.width)
        size = dict(zip("xyz", dims))
        n = [size[d] for d in self.order]
        self.rings = [Ring(self, phase, d, m) for phase, (d, m) in enumerate(zip(self.order, n))]
        first, second, third = self.order
        self.rest = [d for d in "xyz" if d != first]
        self.block = (tuple(size[d] for d in self.rest), (size[third],))
        self.unit = (UNIT[0], self.width)

    def index(self, **at):
        return tuple(at.get(d, slice(None)) for d in "xyz")

    def within(self, b):
        return tuple(b if d == self.order[1] else slice(None) for d in self.rest)

    def events(self, gather):
        rings, direct = [], [("d", self, 2, START, START), ("e", self, 2, START, START)]
        for ring in self.rings[:2][:: -1 if gather else 1]:
            rings.append(("s", self, ring.phase, START, START))
            for j in range(1, ring.steps[NORTH] + gather):
                rings += [("f", self, ring.phase, side, j) for side in (NORTH, SOUTH) if side == NORTH or j < ring.steps[SOUTH] + gather]
            if not gather:
                rings.append(("z", self, ring.phase, START, START))
        return direct + rings if gather else rings + direct


def add_blocks(dst, dst_index, terms, shape):
    def at(ref, index, place):
        place = list(place)
        return ref[tuple([place.pop(0) if isinstance(e, slice) else e for e in index] + place)]

    def row(i, _):
        for rest in [(j,) for n in shape[1:] for j in range(n)] or [()]:
            place = (i, *rest)
            dst[(*dst_index, *place)] = sum(at(ref, index, place).astype(f32) for ref, index in terms).astype(dst.dtype)
        return 0

    lax.fori_loop(0, shape[0], row, 0)


def direct(t, ring, o, w, src, dst, s, slot, half):
    name = ring.name
    return remote(src, dst, s["send" + name].at[half, o - 1], s["recv" + name].at[slot, o - 1], t.beside(ring.d, o))


class Scatter:
    def __init__(self, dims):
        self.colors = [Color(k, dims) for k in range(len(ORDERS))]
        events = [e for c in self.colors for e in c.events(False)]
        times = [time_of(c) for c in SCATTER_TIMES]
        order = sorted(range(len(events)), key=lambda i: (times[i] % SCATTER_STEP, i))
        self.order = [(events[i], times[i] // SCATTER_STEP) for i in order]
        self.depth = max(lag for _, lag in self.order)
        self.slots = self.depth + 1
        ends = [i for i, (e, lag) in enumerate(self.order) if e[0] == "e"]
        self.last = max(ends, key=lambda i: (self.order[i][1], i))
        self.first = min(i for i, (e, lag) in enumerate(self.order) if e[0] == "s" and not e[2])

    def scratch(self):
        shapes = {}
        NS = self.slots
        for c in self.colors:
            for ring in c.rings:
                n, name = ring.n, ring.name
                block = (c.block + ((),))[ring.phase] + c.unit
                shapes["recv" + name] = pltpu.SemaphoreType.DMA((NS, n - 1))
                shapes["send" + name] = pltpu.SemaphoreType.DMA((NS, n - 1))
                shapes["in" + name] = pltpu.VMEM((NS, n - 1) + block, bf16)
                shapes["out" + name] = pltpu.VMEM((self.kept(c, ring.phase, "s" if ring.phase < 2 else "d"), len(ring.sides) if ring.phase < 2 else n - 1) + block, bf16)
                if ring.phase < 2:
                    shapes["sum" + name] = pltpu.VMEM((self.kept(c, ring.phase, "z"),) + block, f32)
            n = c.rings[0].n
            shapes[f"load{c.k}"] = pltpu.VMEM((n, 2) + c.block[0] + c.unit, bf16)
            shapes[f"load_sem{c.k}"] = pltpu.SemaphoreType.DMA((n, 2))
        shapes["part_send"] = pltpu.SemaphoreType.DMA((MATS,))
        shapes["part_recv"] = pltpu.SemaphoreType.DMA((MATS,))
        shapes["free"] = pltpu.SemaphoreType.REGULAR((MATS,))
        return shapes

    def lags(self, c, phase, kinds):
        return [lag for e, lag in self.order if e[1] is c and e[2] == phase and e[0] in kinds]

    def kept(self, c, phase, kind):
        if kind == "s":
            ends = self.lags(c, phase, "z")
        elif kind == "d":
            ends = self.lags(c, phase, "e")
        else:
            ends = self.lags(c, phase + 1, "ze")
        return max(ends) - min(self.lags(c, phase, kind)) + 1

    def bind(self, torus, g, pg, unit, s):
        self.t, self.g, self.pg, self.unit, self.s = torus, g, pg, unit, s

    def partner_copy(self, w):
        t = self.t
        return remote(self.g.at[w, :, :, :, 1 - t.core], self.pg.at[w], self.s["part_send"].at[w], self.s["part_recv"].at[w], t.partner())

    def sign(self, side, w):
        return (1 - 2 * lax.rem(w, 2)) * (1 - 2 * side)

    def target(self, ring, side, j, w):
        return self.t.wrap(ring.d, self.t.at[ring.d] + self.sign(side, w) * (ring.steps[side] - j))

    def loads(self, c, side, j, w):
        ring = c.rings[0]
        place = ring.message(side, j) if j < ring.steps[side] else ring.n - 1
        index = c.index(**{ring.d: self.target(ring, side, j, w)})
        columns = (slice(None), c.columns)
        buf, sem = self.s[f"load{c.k}"], self.s[f"load_sem{c.k}"]
        sources = self.g.at[(w, *index, self.t.core, *columns)], self.pg.at[(w, *index, *columns)]
        return [pltpu.make_async_copy(source, buf.at[place, n], sem.at[place, n]) for n, source in enumerate(sources)]

    def start_loads(self, w):
        for c in self.colors:
            ring = c.rings[0]
            for side in ring.sides:
                for j in range(ring.steps[side] + (side == NORTH)):
                    for copy in self.loads(c, side, j, w):
                        copy.start()

    def message(self, ring, side, m, w, src):
        s, name = self.s, ring.name
        n, slot = ring.message(side, m), lax.rem(w, self.slots)
        return remote(src, s["in" + name].at[slot, n], s["send" + name].at[slot, n], s["recv" + name].at[slot, n], self.t.beside(ring.d, self.sign(side, w)))

    def add(self, dst, index, ring, side, j, w, terms):
        c, s = ring.color, self.s
        if ring.phase:
            before = s["sum" + c.rings[0].name]
            own = [(before, (lax.rem(w, before.shape[0]), *c.within(self.target(ring, side, j, w))))]
        else:
            place = ring.message(side, j) if j < ring.steps[side] else ring.n - 1
            for copy in self.loads(c, side, j, w):
                copy.wait()
            own = [(s[f"load{c.k}"], (place, n)) for n in range(2)]
        add_blocks(dst, index, own + terms, c.block[ring.phase])
        if not ring.phase:

            @pl.when(w + 1 < MATS)
            def _():
                for copy in self.loads(c, side, j, w + 1):
                    copy.start()

    def event(self, kind, c, phase, side, j, w):
        ring, s = c.rings[phase], self.s
        name, slot = ring.name, lax.rem(w, self.slots)
        box, out = s["in" + name], s["out" + name]
        part = lax.rem(w, out.shape[0])
        if kind == "s":
            for side in ring.sides:
                self.add(out, (part, side), ring, side, 0, w, [])
                self.message(ring, side, 0, w, out.at[part, side]).start()
        elif kind == "f":
            at = (slot, ring.message(side, j - 1))
            self.message(ring, side, j - 1, w, out.at[part, 0]).wait_recv()
            self.add(box, at, ring, side, j, w, [(box, at)])
            self.message(ring, side, j, w, box.at[at]).start()
        elif kind == "z":
            terms = []
            for side in ring.sides:
                m = ring.steps[side] - 1
                self.message(ring, side, m, w, out.at[part, 0]).wait_recv()
                terms.append((box, (slot, ring.message(side, m))))
            total = s["sum" + name]
            self.add(total, (lax.rem(w, total.shape[0]),), ring, NORTH, ring.steps[NORTH], w, terms)
            for side in ring.sides:
                for m in range(ring.steps[side]):
                    self.message(ring, side, m, w, out.at[part, 0]).wait_send()
        else:
            total = s["sum" + c.rings[1].name]
            last = lax.rem(w, total.shape[0])
            copies = [direct(self.t, ring, o, w, out.at[part, o - 1], box.at[slot, o - 1], s, slot, slot) for o in range(1, ring.n)]
            if kind == "d":
                for o, copy in enumerate(copies):
                    out[part, o] = total[last, self.t.wrap(ring.d, self.t.at[ring.d] + o + 1)].astype(bf16)
                    copy.start()
            else:
                value = total[last, self.t.at[ring.d]]
                for o, copy in enumerate(copies):
                    copy.wait_recv()
                    value = value + box[slot, o].astype(f32)
                self.unit[w, :, c.columns] = value
                for copy in copies:
                    copy.wait_send()

    def step(self, i):
        @pl.when(i + 1 < MATS)
        def _():
            self.partner_copy(i + 1).wait_recv()

        for n, (e, lag) in enumerate(self.order):
            w = i - lag

            @pl.when((w >= 0) & (w < MATS))
            def _():
                if n == self.first:

                    @pl.when(w >= self.slots)
                    def _():
                        pl.semaphore_wait(self.s["free"].at[w - self.slots], len(self.t.everyone()))

                self.event(*e, w)
                if n == self.last:

                    @pl.when(w + self.slots < MATS)
                    def _():
                        for device in self.t.everyone():
                            signal(self.s["free"].at[w], device)

    def run(self):
        for w in range(MATS):
            self.partner_copy(w).start()
        self.partner_copy(0).wait_recv()
        self.start_loads(0)

        def body(i, _):
            self.step(i)
            return 0

        lax.fori_loop(0, MATS + self.depth, body, 0)
        for w in range(MATS):
            self.partner_copy(w).wait_send()


WAVES = ((1, 1), (0, 1), (0, 3), (1, 0), (0, 0), (0, 2))
SHAPES = (UNIT, DOWN)


def tiles(R, C):
    r, c = TILE
    across, wide = C // c, UNIT[1] // c
    for n in range(R * C // (r * c)):
        yield (pl.ds(n // across * r, r), pl.ds(n % across * c, c)), (pl.ds(n // wide * r, r), pl.ds(n % wide * c, c))


def exchange_scratch():
    shapes = {}
    for kind, (R, C) in enumerate(SHAPES):
        n = sum(w[0] == kind for w in WAVES)
        shapes[f"nat{kind}"] = pltpu.VMEM((R, C), f32)
        shapes[f"slab{kind}"] = pltpu.VMEM((4, n, PADS[kind], C), bf16)
        shapes[f"rows{kind}"] = pltpu.VMEM((4, n, PADS[kind], C), bf16)
    shapes["x_send"] = pltpu.SemaphoreType.DMA((2, 4))
    shapes["x_recv"] = pltpu.SemaphoreType.DMA((2, 4))
    return shapes


def exchange(t, s):
    me = lax.rem(t.idx, 4)
    copies = []
    for o in range(1, 4):
        to = lax.rem(me + o, 4)
        for kind in range(2):
            copies.append(remote(s[f"slab{kind}"].at[to], s[f"rows{kind}"].at[me], s["x_send"].at[kind, o], s["x_recv"].at[kind, o], t.group(to)))
    for copy in copies:
        copy.start()
    for kind in range(2):
        s[f"rows{kind}"][me] = s[f"slab{kind}"][me]
    for copy in copies:
        copy.wait()


def scatter_kernel(dims, names, g, *refs):
    outs, pg, s = refs[:2], refs[2], dict(zip(names, refs[3:], strict=True))
    t = Torus(dims)
    t.enter()
    sc = Scatter(dims)
    sc.bind(t, g, pg, s["unit"], s)
    sc.run()
    for w, (kind, at) in enumerate(WAVES):
        R, C = SHAPES[kind]
        nat, slab = s[f"nat{kind}"], s[f"slab{kind}"]
        for natural, unit in tiles(R, C):
            nat[natural] = s["unit"][(w, *unit)]
        rows = R // 4
        for q in range(4):
            slab[q, at, 0:rows, :] = nat[q * rows : (q + 1) * rows, :].astype(bf16)
    exchange(t, s)
    for kind, out in enumerate(outs):
        C = SHAPES[kind][1]
        for q in range(4):
            out[:, :, C * q : C * (q + 1)] = s[f"rows{kind}"][q]


def places():
    return pl.BlockSpec(memory_space=pl.ANY), pl.BlockSpec(memory_space=pltpu.VMEM)


def scatter(g, dims):
    scratch = Scatter(dims).scratch() | {"unit": pltpu.VMEM((MATS, *UNIT), f32)} | exchange_scratch()
    anywhere, vmem = places()
    rows = [jax.ShapeDtypeStruct((sum(w[0] == kind for w in WAVES), PADS[kind], 4 * C), bf16) for kind, (_, C) in enumerate(SHAPES)]
    *grads, _ = pl.pallas_call(
        functools.partial(scatter_kernel, dims, tuple(scratch)),
        out_shape=(*rows, jax.ShapeDtypeStruct((MATS, *dims, *UNIT), bf16)),
        in_specs=[anywhere],
        out_specs=(vmem, vmem, anywhere),
        scratch_shapes=list(scratch.values()),
        compiler_params=pltpu.CompilerParams(collective_id=1, has_side_effects=True, vmem_limit_bytes=VMEM_MOST),
        name="scatter",
    )(g)
    return grads


class Gather:
    def __init__(self, dims):
        self.colors = [Color(k, dims) for k in range(len(ORDERS))]
        events = [e for c in self.colors for e in c.events(True)]
        timed = []
        for n, (e, character) in enumerate(zip(events, GATHER_TIMES, strict=True)):
            for w in range(MATS):
                timed.append((time_of(character) + GATHER_STEPS[e[2] == START] * w, w, n))
        self.order = [(events[n], w) for _, w, n in sorted(timed)]

    def scratch(self):
        shapes = {}
        for c in self.colors:
            for ring in c.rings:
                for way in ("send", "recv"):
                    shapes[way + ring.name] = pltpu.SemaphoreType.DMA((MATS, ring.n - 1))
        for name in ("over_send", "over_recv"):
            shapes[name] = pltpu.SemaphoreType.DMA((MATS, len(ORDERS)))
        shapes["own"] = pltpu.SemaphoreType.DMA((MATS,))
        return shapes

    def bind(self, torus, out, unit, s):
        self.t, self.out, self.unit, self.s = torus, out, unit, s

    def place(self, c, w, core, **at):
        return self.out.at[(w, *c.index(**at), core, slice(None), c.columns)]

    def own(self, w):
        t = self.t
        return pltpu.make_async_copy(self.unit.at[w], self.out.at[(w, *t.at.values(), t.core)], self.s["own"].at[w])

    def directs(self, ring, w):
        c, t = ring.color, self.t
        src, dst = self.unit.at[w, :, c.columns], self.place(c, w, t.core, **t.at)
        return [direct(t, ring, o, w, src, dst, self.s, w, w) for o in range(1, ring.n)]

    def message(self, ring, side, m, w):
        t, c, s = self.t, ring.color, self.s
        sign = (1 - 2 * side) * (1 - 2 * (w % 2))
        at = {d: t.at[d] for d in c.order[: ring.phase]} | {ring.d: t.wrap(ring.d, t.at[ring.d] - sign * m)}
        block, n = self.place(c, w, t.core, **at), ring.message(side, m)
        return remote(block, block, s["send" + ring.name].at[w, n], s["recv" + ring.name].at[w, n], t.beside(ring.d, sign))

    def over(self, c, w, core, **at):
        block = self.place(c, w, core, **at)
        return remote(block, block, self.s["over_send"].at[w, c.k], self.s["over_recv"].at[w, c.k], self.t.partner())

    def event(self, kind, c, phase, side, j, w):
        ring, t = c.rings[phase], self.t
        if kind == "d":
            for copy in self.directs(ring, w):
                copy.start()
        elif kind == "e":
            for copy in self.directs(ring, w):
                copy.wait_recv()
        elif kind == "s":
            for side in ring.sides:
                self.message(ring, side, 0, w).start()
            if not phase:
                self.over(c, w, t.core, **{ring.d: t.at[ring.d]}).start()
        else:
            self.message(ring, side, j - 1, w).wait_recv()
            if j < ring.steps[side]:
                self.message(ring, side, j, w).start()
            if not phase:
                sign = (1 - 2 * side) * (1 - 2 * (w % 2))
                self.over(c, w, t.core, **{ring.d: t.wrap(ring.d, t.at[ring.d] - sign * j)}).start()

    def finish(self, w):
        for c in self.colors:
            for ring in c.rings:
                if ring.phase == 2:
                    for copy in self.directs(ring, w):
                        copy.wait_send()
                else:
                    for side in ring.sides:
                        for m in range(ring.steps[side]):
                            self.message(ring, side, m, w).wait_send()
            self.over(c, w, self.t.core).wait_send()
            self.over(c, w, 1 - self.t.core).wait_recv()

    def run(self):
        for w in range(MATS):
            self.own(w).wait()
        for e, w in self.order:
            self.event(*e, w)
        for w in range(MATS):
            self.finish(w)


AXES = ("core", "x", "y", "z")


def sum_over_all(t, s, value):
    for n, d in enumerate(AXES):
        mine, box = s["norm_out"].at[n], s["norm_" + d]
        mine[...] = value
        copies = []
        for o in range(box.shape[0]):
            device = t.partner() if d == "core" else t.beside(d, o + 1)
            copies.append(remote(mine, box.at[o], s["norm_send"].at[n, o], s["norm_recv"].at[n, o], device))
        for copy in copies:
            copy.start()
        for copy in copies:
            copy.wait()
        for o in range(box.shape[0]):
            value = value + box[o]
    return value


def update_kernel(dims, names, *refs):
    take = iter(refs)
    grads, w_in, m_in, v_in, m_out, v_out = ([next(take) for _ in range(n)] for n in (2, 3, 3, 3, 3, 3))
    out = next(take)
    s = dict(zip(names, take, strict=True))
    t = Torus(dims)
    t.enter()

    def rows(kind, at):
        return grads[kind][at, 0 : SHAPES[kind][0] // 4, :].astype(f32)

    total, count = jnp.zeros((1, 1), f32), 0
    for kind, at in WAVES:
        g = rows(kind, at)
        count += g.size
        total = total + jnp.sum(jnp.sum(g * g, axis=0, keepdims=True), axis=1, keepdims=True)
    for d in AXES:
        count *= s["norm_" + d].shape[0] + 1
    total = sum_over_all(t, s, jnp.broadcast_to(total, TILE))[0:1, 0:1]
    factor = jnp.minimum(1.0, 0.5 * lax.rsqrt(total / count + 1e-30))

    for kind, at in WAVES:
        which, layer = (2, at) if kind else divmod(at, 2)
        R, C = SHAPES[kind]
        g = rows(kind, at) * factor
        w = w_in[which][layer].astype(f32)
        m = 0.9 * m_in[which][layer] + 0.1 * g
        v = 0.95 * v_in[which][layer] + 0.05 * g * g
        m_out[which][layer] = m
        v_out[which][layer] = v
        w = (w - 0.02 * (m * lax.rsqrt(v + 1e-8) + 0.1 * w)).astype(bf16)
        for q in range(4):
            s[f"slab{kind}"][q, at, 0 : R // 4, :] = w[:, C * q : C * (q + 1)]
    exchange(t, s)
    ga = Gather(dims)
    ga.bind(t, out, s["unit"], s)
    for w, (kind, at) in enumerate(WAVES):
        R, C = SHAPES[kind]
        nat, rows_in, n = s[f"nat{kind}"], s[f"rows{kind}"], R // 4
        for q in range(4):
            nat[q * n : (q + 1) * n, :] = rows_in[q, at, 0:n, :].astype(f32)
        for natural, unit in tiles(R, C):
            s["wide"][unit] = nat[natural]
        s["unit"][w] = s["wide"][...].astype(bf16)
        ga.own(w).start()
    ga.run()


def update(grads, w, m, v, dims):
    scratch = Gather(dims).scratch() | exchange_scratch()
    scratch["unit"] = pltpu.VMEM((MATS, *UNIT), bf16)
    scratch["wide"] = pltpu.VMEM(UNIT, f32)
    scratch["norm_out"] = pltpu.VMEM((len(AXES), *TILE), f32)
    for d, n in zip(AXES, (2, *dims), strict=True):
        scratch["norm_" + d] = pltpu.VMEM((n - 1, *TILE), f32)
    for name in ("norm_send", "norm_recv"):
        scratch[name] = pltpu.SemaphoreType.DMA((len(AXES), max(dims)))
    anywhere, vmem = places()
    given = (*grads, *w, *m, *v)
    like = [jax.ShapeDtypeStruct(a.shape, f32) for a in (*m, *v)]
    *mv, out = pl.pallas_call(
        functools.partial(update_kernel, dims, tuple(scratch)),
        out_shape=(*like, jax.ShapeDtypeStruct((MATS, *dims, 2, *UNIT), bf16)),
        in_specs=[vmem] * len(given),
        out_specs=(*[vmem] * len(like), anywhere),
        scratch_shapes=list(scratch.values()),
        compiler_params=pltpu.CompilerParams(collective_id=2, has_side_effects=True, vmem_limit_bytes=VMEM_SOME),
        name="update",
    )(*given)
    return mv, out


VMEM_MOST, VMEM_SOME = 62 << 20, 40 << 20


def normed(h):
    wide = h.astype(f32)
    scale = lax.rsqrt(jnp.mean(wide**2, -1, keepdims=True) + 1e-6)
    return (wide * scale).astype(bf16)


def dotf(a, b, dims):
    return lax.dot_general(a, b, (dims, ((), ())), preferred_element_type=f32)


def glu(gate, up):
    return jax.nn.silu(gate) * up


def enter_layer(h, wg, wu):
    a, norm_back = jax.vjp(normed, h)
    gate = dotf(a, wg, ((1,), (0,)))
    up = dotf(a, wu, ((1,), (0,)))
    return a, gate, up, lax.optimization_barrier(glu(gate, up).astype(bf16)), norm_back


def back_to_hidden(dh, gate, up, wd):
    dhid = dotf(dh, wd, ((1,), (1,))).astype(bf16).astype(f32)
    dgate, dup = jax.vjp(glu, gate, up)[1](dhid)
    return dgate.astype(bf16), dup.astype(bf16)


def factors(x, dy, wg, wu, wd):
    a0, gate0, up0, hid0, _ = enter_layer(x, wg[0], wu[0])
    h1 = x + dotf(hid0, wd[0], ((1,), (0,))).astype(bf16)
    a1, gate1, up1, hid1, norm_back = enter_layer(h1, wg[1], wu[1])
    dg1, du1 = back_to_hidden(dy, gate1, up1, wd[1])
    da = dotf(dg1, wg[1], ((1,), (1,))).astype(bf16) + dotf(du1, wu[1], ((1,), (1,))).astype(bf16)
    dh1 = dy + norm_back(da)[0]
    dg0, du0 = back_to_hidden(dh1, gate0, up0, wd[0])
    return (hid1, dy), (a1, dg1), (a1, du1), (hid0, dh1), (a0, dg0), (a0, du0)


def product_kernel(kind, left, right, *refs):
    out = refs[-1]
    C, width = SHAPES[kind][1], out.shape[5] * SHAPES[kind][1]
    for start in range(0, width, CHUNK):
        wide = lax.dot_general(left[...], right[:, start : start + CHUNK], (((0,), (0,)), ((), ())), preferred_element_type=f32)
        wide = wide.reshape(out.shape[2], out.shape[3], SHAPES[kind][0], CHUNK)
        if kind:
            for natural, unit in tiles(*DOWN):
                for core in range(out.shape[5]):
                    at = core * C + natural[1].start - start
                    if 0 <= at < CHUNK:
                        out[(0, 0, slice(None), slice(None), 0, core, *unit)] = wide[:, :, natural[0].start : natural[0].start + natural[0].size, at : at + natural[1].size].astype(bf16)
        else:
            for core in range(out.shape[5]):
                begin, end = max(start, core * C), min(start + CHUNK, core * C + C)
                if begin < end:
                    out[0, 0, :, :, 0, core, :, begin - core * C : end - core * C] = wide[..., begin - start : end - start].astype(bf16)


CHUNK = 256


def product(wave, left, right, into, dims):
    X, Y, Z = dims
    kind = WAVES[wave][0]
    R, C = SHAPES[kind]
    tokens, halves = right.shape[0], Z // 2
    given = [] if into is None else [into]
    return pl.pallas_call(
        functools.partial(product_kernel, kind),
        grid=(2, X),
        out_shape=jax.ShapeDtypeStruct((MATS, X, Y, halves, 2, 2, *UNIT), bf16),
        in_specs=[pl.BlockSpec((tokens, R * Y * halves), lambda p, i: (0, i)), pl.BlockSpec((tokens, 2 * C), lambda p, i: (0, p))]
        + [pl.BlockSpec(memory_space=pl.ANY)] * len(given),
        out_specs=pl.BlockSpec((1, 1, Y, halves, 1, 2, *UNIT), lambda p, i: (wave, i, 0, 0, p, 0, 0, 0)),
        input_output_aliases={2: 0} if given else {},
        cost_estimate=pl.CostEstimate(flops=2 * left.size * right.shape[1], bytes_accessed=2 * left.shape[1] * right.shape[1], transcendentals=0),
        compiler_params=pltpu.CompilerParams(vmem_limit_bytes=VMEM_SOME),
        name="product",
    )(left, right, *given)


def settle_kernel(kind, w, out):
    R, C = SHAPES[kind]
    for p in range(2):
        for core in range(2):
            q = 2 * p + core
            block = w.at[0, 0, :, :, p, core]
            if kind:
                for natural, unit in tiles(*DOWN):
                    out[:, :, :, natural[0], pl.ds(C * q + natural[1].start, natural[1].size)] = block[(slice(None), slice(None), *unit)][None]
            else:
                out[:, :, :, :, C * q : C * (q + 1)] = block[...][None]


def settle(w, waves, dims):
    X, Y, Z = dims
    kind = WAVES[waves[0]][0]
    R, C = SHAPES[kind]
    halves = Z // 2
    out = pl.pallas_call(
        functools.partial(settle_kernel, kind),
        grid=(2, X),
        out_shape=jax.ShapeDtypeStruct((2, X * Y, halves, R, 4 * C), bf16),
        in_specs=[pl.BlockSpec((1, 1, Y, halves, 2, 2, *UNIT), lambda n, i: (waves[0] + (waves[1] - waves[0]) * n, i, 0, 0, 0, 0, 0, 0))],
        out_specs=pl.BlockSpec((1, Y, halves, R, 4 * C), lambda n, i: (n, i, 0, 0, 0)),
        compiler_params=pltpu.CompilerParams(vmem_limit_bytes=VMEM_SOME),
        name="settle",
    )(w)
    return out.reshape(2, -1, 4 * C)


def device_step(dims, x, dy, wg, wu, wd, *moments):
    X, Y, Z = dims
    m, v = moments[:3], moments[3:]
    g = None
    for wave, (left, right) in enumerate(factors(x[0], dy[0], wg, wu, wd)):
        g = product(wave, left, right, g, dims)
    grads = scatter(g.reshape(MATS, *dims, 2, *UNIT), dims)
    place = lax.axis_index("dp")
    w = [lax.dynamic_slice_in_dim(a, place * b.shape[1], b.shape[1], 1) for a, b in zip((wg, wu, wd), m, strict=True)]
    mv, out = update(grads, w, m, v, dims)
    out = out.reshape(MATS, X, Y, Z // 2, 2, 2, *UNIT)
    waves = [[WAVES.index((1, n) if which == 2 else (0, 2 * which + n)) for n in range(2)] for which in range(3)]
    return (*[settle(out, pair, dims) for pair in waves], *mv)


DIMS = {256: (4, 4, 8)}


def solution(mesh):
    dims = DIMS[mesh.shape["dp"]]
    spec = jax.sharding.PartitionSpec
    tokens, whole, rows = spec(("rep", "dp")), spec(), spec(None, "dp", None)
    return jax.shard_map(
        functools.partial(device_step, dims),
        mesh=mesh,
        in_specs=(tokens, tokens, *[whole] * 3, *[rows] * 6),
        out_specs=(*[spec("rep")] * 3, *[spec("rep", "dp", None)] * 6),
        check_vma=False,
    )
```

```python
import functools
import jax, jax.numpy as jnp
from jax import lax
from jax.experimental import pallas as pl
from jax.experimental.pallas import tpu as pltpu

bf16, f32 = jnp.bfloat16, jnp.float32
MATS = 6
UNIT = (24, 896)
DOWN = (56, 384)
TILE = (8, 128)
PADS = (8, 16)
ORDERS = ("xyz", "yzx", "zxy")
COLUMNS = ((0, 384), (384, 256), (640, 256))
KINDS = ("s", "f", "z", "d", "e")
SCATTER_TIMES, SCATTER_STEP = "#:LMWbb{'6CCMMXaajjs#/'85CTT]ghq", 18
GATHER_TIMES, GATHER_STEPS = '#-.4799Yj~#337;<DEOPQ_oi#((3@AAKX\\bgoy', (4, 14)
MESH = pl.DeviceIdType.MESH
START, MORE = 0, 1
NORTH, SOUTH = 0, 1


def time_of(character):
    return ord(character) - ord("#")


class Torus:
    def __init__(self, dims):
        self.dims = dict(zip("xyz", dims))
        self.cores = 2
        _, Y, Z = dims
        self.stride = dict(zip("xyz", (Y * Z * self.cores, Z * self.cores, self.cores)))
        self.rep, self.idx = lax.axis_index("rep"), lax.axis_index("dp")
        self.at = {d: lax.rem(lax.div(self.idx, self.stride[d]), self.dims[d]) for d in "xyz"}
        self.core = lax.rem(self.idx, self.cores)

    def wrap(self, d, value):
        n = self.dims[d]
        return lax.rem(value + n, n)

    def beside(self, d, offset):
        return (self.rep, self.idx + (self.wrap(d, self.at[d] + offset) - self.at[d]) * self.stride[d])

    def partner(self):
        return (self.rep, self.idx + 1 - 2 * self.core)

    def everyone(self):
        return [self.beside(d, o) for d in "xyz" for o in range(1, self.dims[d])]

    def group(self, s):
        return (self.rep, self.idx - lax.rem(self.idx, 4) + s)

    def enter(self):
        me = lax.rem(self.idx, 4)
        barrier = pltpu.get_barrier_semaphore()
        devices = self.everyone() + [self.partner(), self.group(lax.rem(me + 3 - 2 * self.core, 4))]
        for device in devices:
            signal(barrier, device)
        pl.semaphore_wait(barrier, len(devices))


def signal(sem, device):
    pl.semaphore_signal(sem, inc=1, device_id=device, device_id_type=MESH)


def remote(src, dst, send, recv, device):
    return pltpu.make_async_remote_copy(src_ref=src, dst_ref=dst, send_sem=send, recv_sem=recv, device_id=device, device_id_type=MESH)


class Ring:
    def __init__(self, color, phase, d, n):
        self.name = f"{color.k}{phase}"
        self.color, self.phase, self.d, self.n = color, phase, d, n
        self.steps = (n // 2, (n - 1) // 2)
        self.sides = [side for side in (NORTH, SOUTH) if self.steps[side]]

    def message(self, side, m):
        return m + side * self.steps[NORTH]


class Color:
    def __init__(self, k, dims):
        self.k, self.order = k, ORDERS[k]
        start, self.width = COLUMNS[k]
        self.columns = pl.ds(start, self.width)
        size = dict(zip("xyz", dims))
        n = [size[d] for d in self.order]
        self.rings = [Ring(self, phase, d, m) for phase, (d, m) in enumerate(zip(self.order, n))]
        first, second, third = self.order
        self.rest = [d for d in "xyz" if d != first]
        self.block = (tuple(size[d] for d in self.rest), (size[third],))
        self.unit = (UNIT[0], self.width)

    def index(self, **at):
        return tuple(at.get(d, slice(None)) for d in "xyz")

    def within(self, b):
        return tuple(b if d == self.order[1] else slice(None) for d in self.rest)

    def events(self, gather):
        rings, direct = [], [("d", self, 2, START, START), ("e", self, 2, START, START)]
        for ring in self.rings[:2][:: -1 if gather else 1]:
            rings.append(("s", self, ring.phase, START, START))
            for j in range(1, ring.steps[NORTH] + gather):
                rings += [("f", self, ring.phase, side, j) for side in (NORTH, SOUTH) if side == NORTH or j < ring.steps[SOUTH] + gather]
            if not gather:
                rings.append(("z", self, ring.phase, START, START))
        return direct + rings if gather else rings + direct


def add_blocks(dst, dst_index, terms, shape):
    def at(ref, index, place):
        place = list(place)
        return ref[tuple([place.pop(0) if isinstance(e, slice) else e for e in index] + place)]

    def row(i, _):
        for rest in [(j,) for n in shape[1:] for j in range(n)] or [()]:
            place = (i, *rest)
            dst[(*dst_index, *place)] = sum(at(ref, index, place).astype(f32) for ref, index in terms).astype(dst.dtype)
        return 0

    lax.fori_loop(0, shape[0], row, 0)


def direct(t, ring, o, w, src, dst, s, slot, half):
    name = ring.name
    return remote(src, dst, s["send" + name].at[half, o - 1], s["recv" + name].at[slot, o - 1], t.beside(ring.d, o))


class Scatter:
    def __init__(self, dims):
        self.colors = [Color(k, dims) for k in range(len(ORDERS))]
        events = [e for c in self.colors for e in c.events(False)]
        times = [time_of(c) for c in SCATTER_TIMES]
        order = sorted(range(len(events)), key=lambda i: (times[i] % SCATTER_STEP, i))
        self.order = [(events[i], times[i] // SCATTER_STEP) for i in order]
        self.depth = max(lag for _, lag in self.order)
        self.slots = self.depth + 1
        ends = [i for i, (e, lag) in enumerate(self.order) if e[0] == "e"]
        self.last = max(ends, key=lambda i: (self.order[i][1], i))
        self.first = min(i for i, (e, lag) in enumerate(self.order) if e[0] == "s" and not e[2])

    def scratch(self):
        shapes = {}
        NS = self.slots
        for c in self.colors:
            for ring in c.rings:
                n, name = ring.n, ring.name
                block = (c.block + ((),))[ring.phase] + c.unit
                shapes["recv" + name] = pltpu.SemaphoreType.DMA((NS, n - 1))
                shapes["send" + name] = pltpu.SemaphoreType.DMA((NS, n - 1))
                shapes["in" + name] = pltpu.VMEM((NS, n - 1) + block, bf16)
                shapes["out" + name] = pltpu.VMEM((self.kept(c, ring.phase, "s" if ring.phase < 2 else "d"), len(ring.sides) if ring.phase < 2 else n - 1) + block, bf16)
                if ring.phase < 2:
                    shapes["sum" + name] = pltpu.VMEM((self.kept(c, ring.phase, "z"),) + block, f32)
            n = c.rings[0].n
            shapes[f"load{c.k}"] = pltpu.VMEM((n, 2) + c.block[0] + c.unit, bf16)
            shapes[f"load_sem{c.k}"] = pltpu.SemaphoreType.DMA((n, 2))
        shapes["part_send"] = pltpu.SemaphoreType.DMA((MATS,))
        shapes["part_recv"] = pltpu.SemaphoreType.DMA((MATS,))
        shapes["free"] = pltpu.SemaphoreType.REGULAR((MATS,))
        return shapes

    def lags(self, c, phase, kinds):
        return [lag for e, lag in self.order if e[1] is c and e[2] == phase and e[0] in kinds]

    def kept(self, c, phase, kind):
        if kind == "s":
            ends = self.lags(c, phase, "z")
        elif kind == "d":
            ends = self.lags(c, phase, "e")
        else:
            ends = self.lags(c, phase + 1, "ze")
        return max(ends) - min(self.lags(c, phase, kind)) + 1

    def bind(self, torus, g, pg, unit, s):
        self.t, self.g, self.pg, self.unit, self.s = torus, g, pg, unit, s

    def partner_copy(self, w):
        t = self.t
        return remote(self.g.at[w, :, :, :, 1 - t.core], self.pg.at[w], self.s["part_send"].at[w], self.s["part_recv"].at[w], t.partner())

    def sign(self, side, w):
        return (1 - 2 * lax.rem(w, 2)) * (1 - 2 * side)

    def target(self, ring, side, j, w):
        return self.t.wrap(ring.d, self.t.at[ring.d] + self.sign(side, w) * (ring.steps[side] - j))

    def loads(self, c, side, j, w):
        ring = c.rings[0]
        place = ring.message(side, j) if j < ring.steps[side] else ring.n - 1
        index = c.index(**{ring.d: self.target(ring, side, j, w)})
        columns = (slice(None), c.columns)
        buf, sem = self.s[f"load{c.k}"], self.s[f"load_sem{c.k}"]
        sources = self.g.at[(w, *index, self.t.core, *columns)], self.pg.at[(w, *index, *columns)]
        return [pltpu.make_async_copy(source, buf.at[place, n], sem.at[place, n]) for n, source in enumerate(sources)]

    def start_loads(self, w):
        for c in self.colors:
            ring = c.rings[0]
            for side in ring.sides:
                for j in range(ring.steps[side] + (side == NORTH)):
                    for copy in self.loads(c, side, j, w):
                        copy.start()

    def message(self, ring, side, m, w, src):
        s, name = self.s, ring.name
        n, slot = ring.message(side, m), lax.rem(w, self.slots)
        return remote(src, s["in" + name].at[slot, n], s["send" + name].at[slot, n], s["recv" + name].at[slot, n], self.t.beside(ring.d, self.sign(side, w)))

    def add(self, dst, index, ring, side, j, w, terms):
        c, s = ring.color, self.s
        if ring.phase:
            before = s["sum" + c.rings[0].name]
            own = [(before, (lax.rem(w, before.shape[0]), *c.within(self.target(ring, side, j, w))))]
        else:
            place = ring.message(side, j) if j < ring.steps[side] else ring.n - 1
            for copy in self.loads(c, side, j, w):
                copy.wait()
            own = [(s[f"load{c.k}"], (place, n)) for n in range(2)]
        add_blocks(dst, index, own + terms, c.block[ring.phase])
        if not ring.phase:

            @pl.when(w + 1 < MATS)
            def _():
                for copy in self.loads(c, side, j, w + 1):
                    copy.start()

    def event(self, kind, c, phase, side, j, w):
        ring, s = c.rings[phase], self.s
        name, slot = ring.name, lax.rem(w, self.slots)
        box, out = s["in" + name], s["out" + name]
        part = lax.rem(w, out.shape[0])
        if kind == "s":
            for side in ring.sides:
                self.add(out, (part, side), ring, side, 0, w, [])
                self.message(ring, side, 0, w, out.at[part, side]).start()
        elif kind == "f":
            at = (slot, ring.message(side, j - 1))
            self.message(ring, side, j - 1, w, out.at[part, 0]).wait_recv()
            self.add(box, at, ring, side, j, w, [(box, at)])
            self.message(ring, side, j, w, box.at[at]).start()
        elif kind == "z":
            terms = []
            for side in ring.sides:
                m = ring.steps[side] - 1
                self.message(ring, side, m, w, out.at[part, 0]).wait_recv()
                terms.append((box, (slot, ring.message(side, m))))
            total = s["sum" + name]
            self.add(total, (lax.rem(w, total.shape[0]),), ring, NORTH, ring.steps[NORTH], w, terms)
            for side in ring.sides:
                for m in range(ring.steps[side]):
                    self.message(ring, side, m, w, out.at[part, 0]).wait_send()
        else:
            total = s["sum" + c.rings[1].name]
            last = lax.rem(w, total.shape[0])
            copies = [direct(self.t, ring, o, w, out.at[part, o - 1], box.at[slot, o - 1], s, slot, slot) for o in range(1, ring.n)]
            if kind == "d":
                for o, copy in enumerate(copies):
                    out[part, o] = total[last, self.t.wrap(ring.d, self.t.at[ring.d] + o + 1)].astype(bf16)
                    copy.start()
            else:
                value = total[last, self.t.at[ring.d]]
                for o, copy in enumerate(copies):
                    copy.wait_recv()
                    value = value + box[slot, o].astype(f32)
                self.unit[w, :, c.columns] = value
                for copy in copies:
                    copy.wait_send()

    def step(self, i):
        @pl.when(i + 1 < MATS)
        def _():
            self.partner_copy(i + 1).wait_recv()

        for n, (e, lag) in enumerate(self.order):
            w = i - lag

            @pl.when((w >= 0) & (w < MATS))
            def _():
                if n == self.first:

                    @pl.when(w >= self.slots)
                    def _():
                        pl.semaphore_wait(self.s["free"].at[w - self.slots], len(self.t.everyone()))

                self.event(*e, w)
                if n == self.last:

                    @pl.when(w + self.slots < MATS)
                    def _():
                        for device in self.t.everyone():
                            signal(self.s["free"].at[w], device)

    def run(self):
        for w in range(MATS):
            self.partner_copy(w).start()
        self.partner_copy(0).wait_recv()
        self.start_loads(0)

        def body(i, _):
            self.step(i)
            return 0

        lax.fori_loop(0, MATS + self.depth, body, 0)
        for w in range(MATS):
            self.partner_copy(w).wait_send()


WAVES = ((1, 1), (0, 1), (0, 3), (1, 0), (0, 0), (0, 2))
SHAPES = (UNIT, DOWN)


def tiles(R, C):
    r, c = TILE
    across, wide = C // c, UNIT[1] // c
    for n in range(R * C // (r * c)):
        yield (pl.ds(n // across * r, r), pl.ds(n % across * c, c)), (pl.ds(n // wide * r, r), pl.ds(n % wide * c, c))


def exchange_scratch():
    shapes = {}
    for kind, (R, C) in enumerate(SHAPES):
        n = sum(w[0] == kind for w in WAVES)
        shapes[f"nat{kind}"] = pltpu.VMEM((R, C), f32)
        shapes[f"slab{kind}"] = pltpu.VMEM((4, n, PADS[kind], C), bf16)
        shapes[f"rows{kind}"] = pltpu.VMEM((4, n, PADS[kind], C), bf16)
    shapes["x_send"] = pltpu.SemaphoreType.DMA((2, 4))
    shapes["x_recv"] = pltpu.SemaphoreType.DMA((2, 4))
    return shapes


def exchange(t, s):
    me = lax.rem(t.idx, 4)
    copies = []
    for o in range(1, 4):
        to = lax.rem(me + o, 4)
        for kind in range(2):
            copies.append(remote(s[f"slab{kind}"].at[to], s[f"rows{kind}"].at[me], s["x_send"].at[kind, o], s["x_recv"].at[kind, o], t.group(to)))
    for copy in copies:
        copy.start()
    for kind in range(2):
        s[f"rows{kind}"][me] = s[f"slab{kind}"][me]
    for copy in copies:
        copy.wait()


def scatter_kernel(dims, names, g, *refs):
    outs, pg, s = refs[:2], refs[2], dict(zip(names, refs[3:], strict=True))
    t = Torus(dims)
    t.enter()
    sc = Scatter(dims)
    sc.bind(t, g, pg, s["unit"], s)
    sc.run()
    for w, (kind, at) in enumerate(WAVES):
        R, C = SHAPES[kind]
        nat, slab = s[f"nat{kind}"], s[f"slab{kind}"]
        for natural, unit in tiles(R, C):
            nat[natural] = s["unit"][(w, *unit)]
        rows = R // 4
        for q in range(4):
            slab[q, at, 0:rows, :] = nat[q * rows : (q + 1) * rows, :].astype(bf16)
    exchange(t, s)
    for kind, out in enumerate(outs):
        C = SHAPES[kind][1]
        for q in range(4):
            out[:, :, C * q : C * (q + 1)] = s[f"rows{kind}"][q]


def places():
    return pl.BlockSpec(memory_space=pl.ANY), pl.BlockSpec(memory_space=pltpu.VMEM)


def scatter(g, dims):
    scratch = Scatter(dims).scratch() | {"unit": pltpu.VMEM((MATS, *UNIT), f32)} | exchange_scratch()
    anywhere, vmem = places()
    rows = [jax.ShapeDtypeStruct((sum(w[0] == kind for w in WAVES), PADS[kind], 4 * C), bf16) for kind, (_, C) in enumerate(SHAPES)]
    *grads, _ = pl.pallas_call(
        functools.partial(scatter_kernel, dims, tuple(scratch)),
        out_shape=(*rows, jax.ShapeDtypeStruct((MATS, *dims, *UNIT), bf16)),
        in_specs=[anywhere],
        out_specs=(vmem, vmem, anywhere),
        scratch_shapes=list(scratch.values()),
        compiler_params=pltpu.CompilerParams(collective_id=1, has_side_effects=True, vmem_limit_bytes=VMEM_MOST),
        name="scatter",
    )(g)
    return grads


class Gather:
    def __init__(self, dims):
        self.colors = [Color(k, dims) for k in range(len(ORDERS))]
        events = [e for c in self.colors for e in c.events(True)]
        timed = []
        for n, (e, character) in enumerate(zip(events, GATHER_TIMES, strict=True)):
            for w in range(MATS):
                timed.append((time_of(character) + GATHER_STEPS[e[2] == START] * w, w, n))
        self.order = [(events[n], w) for _, w, n in sorted(timed)]

    def scratch(self):
        shapes = {}
        for c in self.colors:
            for ring in c.rings:
                for way in ("send", "recv"):
                    shapes[way + ring.name] = pltpu.SemaphoreType.DMA((MATS, ring.n - 1))
        for name in ("over_send", "over_recv"):
            shapes[name] = pltpu.SemaphoreType.DMA((MATS, len(ORDERS)))
        shapes["own"] = pltpu.SemaphoreType.DMA((MATS,))
        return shapes

    def bind(self, torus, out, unit, s):
        self.t, self.out, self.unit, self.s = torus, out, unit, s

    def place(self, c, w, core, **at):
        return self.out[w].at[(*c.index(**at), core, slice(None), c.columns)]

    def own(self, w):
        t = self.t
        return pltpu.make_async_copy(self.unit.at[w], self.out[w].at[(*t.at.values(), t.core)], self.s["own"].at[w])

    def directs(self, ring, w):
        c, t = ring.color, self.t
        src, dst = self.unit.at[w, :, c.columns], self.place(c, w, t.core, **t.at)
        return [direct(t, ring, o, w, src, dst, self.s, w, w) for o in range(1, ring.n)]

    def message(self, ring, side, m, w):
        t, c, s = self.t, ring.color, self.s
        sign = (1 - 2 * side) * (1 - 2 * (w % 2))
        at = {d: t.at[d] for d in c.order[: ring.phase]} | {ring.d: t.wrap(ring.d, t.at[ring.d] - sign * m)}
        block, n = self.place(c, w, t.core, **at), ring.message(side, m)
        return remote(block, block, s["send" + ring.name].at[w, n], s["recv" + ring.name].at[w, n], t.beside(ring.d, sign))

    def over(self, c, w, core, **at):
        block = self.place(c, w, core, **at)
        return remote(block, block, self.s["over_send"].at[w, c.k], self.s["over_recv"].at[w, c.k], self.t.partner())

    def event(self, kind, c, phase, side, j, w):
        ring, t = c.rings[phase], self.t
        if kind == "d":
            for copy in self.directs(ring, w):
                copy.start()
        elif kind == "e":
            for copy in self.directs(ring, w):
                copy.wait_recv()
        elif kind == "s":
            for side in ring.sides:
                self.message(ring, side, 0, w).start()
            if not phase:
                self.over(c, w, t.core, **{ring.d: t.at[ring.d]}).start()
        else:
            self.message(ring, side, j - 1, w).wait_recv()
            if j < ring.steps[side]:
                self.message(ring, side, j, w).start()
            if not phase:
                sign = (1 - 2 * side) * (1 - 2 * (w % 2))
                self.over(c, w, t.core, **{ring.d: t.wrap(ring.d, t.at[ring.d] - sign * j)}).start()

    def finish(self, w):
        for c in self.colors:
            for ring in c.rings:
                if ring.phase == 2:
                    for copy in self.directs(ring, w):
                        copy.wait_send()
                else:
                    for side in ring.sides:
                        for m in range(ring.steps[side]):
                            self.message(ring, side, m, w).wait_send()
            self.over(c, w, self.t.core).wait_send()
            self.over(c, w, 1 - self.t.core).wait_recv()

    def run(self):
        for w in range(MATS):
            self.own(w).wait()
        for e, w in self.order:
            self.event(*e, w)
        for w in range(MATS):
            self.finish(w)


AXES = ("core", "x", "y", "z")


def sum_over_all(t, s, value):
    for n, d in enumerate(AXES):
        mine, box = s["norm_out"].at[n], s["norm_" + d]
        mine[...] = value
        copies = []
        for o in range(box.shape[0]):
            device = t.partner() if d == "core" else t.beside(d, o + 1)
            copies.append(remote(mine, box.at[o], s["norm_send"].at[n, o], s["norm_recv"].at[n, o], device))
        for copy in copies:
            copy.start()
        for copy in copies:
            copy.wait()
        for o in range(box.shape[0]):
            value = value + box[o]
    return value


def update_kernel(dims, names, *refs):
    take = iter(refs)
    grads, w_in, m_in, v_in, m_out, v_out = ([next(take) for _ in range(n)] for n in (2, 3, 3, 3, 3, 3))
    out = [next(take) for _ in WAVES]
    s = dict(zip(names, take, strict=True))
    t = Torus(dims)
    t.enter()

    def rows(kind, at):
        return grads[kind][at, 0 : SHAPES[kind][0] // 4, :].astype(f32)

    total, count = jnp.zeros((1, 1), f32), 0
    for kind, at in WAVES:
        g = rows(kind, at)
        count += g.size
        total = total + jnp.sum(jnp.sum(g * g, axis=0, keepdims=True), axis=1, keepdims=True)
    for d in AXES:
        count *= s["norm_" + d].shape[0] + 1
    total = sum_over_all(t, s, jnp.broadcast_to(total, TILE))[0:1, 0:1]
    factor = jnp.minimum(1.0, 0.5 * lax.rsqrt(total / count + 1e-30))

    for kind, at in WAVES:
        which, layer = (2, at) if kind else divmod(at, 2)
        R, C = SHAPES[kind]
        g = rows(kind, at) * factor
        w = w_in[which][layer].astype(f32)
        m = 0.9 * m_in[which][:, layer, :] + 0.1 * g
        v = 0.95 * v_in[which][:, layer, :] + 0.05 * g * g
        m_out[which][:, layer, :] = m
        v_out[which][:, layer, :] = v
        w = (w - 0.02 * (m * lax.rsqrt(v + 1e-8) + 0.1 * w)).astype(bf16)
        for q in range(4):
            s[f"slab{kind}"][q, at, 0 : R // 4, :] = w[:, C * q : C * (q + 1)]
    exchange(t, s)
    ga = Gather(dims)
    ga.bind(t, out, s["unit"], s)
    for w, (kind, at) in enumerate(WAVES):
        R, C = SHAPES[kind]
        nat, rows_in, n = s[f"nat{kind}"], s[f"rows{kind}"], R // 4
        for q in range(4):
            nat[q * n : (q + 1) * n, :] = rows_in[q, at, 0:n, :].astype(f32)
        for natural, unit in tiles(R, C):
            s["wide"][unit] = nat[natural]
        s["unit"][w] = s["wide"][...].astype(bf16)
        ga.own(w).start()
    ga.run()


IN_VMEM = (1, 2, 4)


def home(wave):
    return pltpu.VMEM if wave in IN_VMEM else pltpu.HBM


def update(grads, w, moments, dims):
    scratch = Gather(dims).scratch() | exchange_scratch()
    scratch["unit"] = pltpu.VMEM((MATS, *UNIT), bf16)
    scratch["wide"] = pltpu.VMEM(UNIT, f32)
    scratch["norm_out"] = pltpu.VMEM((len(AXES), *TILE), f32)
    for d, n in zip(AXES, (2, *dims), strict=True):
        scratch["norm_" + d] = pltpu.VMEM((n - 1, *TILE), f32)
    for name in ("norm_send", "norm_recv"):
        scratch[name] = pltpu.SemaphoreType.DMA((len(AXES), max(dims)))
    anywhere, vmem = places()
    given = (*grads, *w, *moments)
    like = [jax.ShapeDtypeStruct(a.shape, f32) for a in moments]
    results = pl.pallas_call(
        functools.partial(update_kernel, dims, tuple(scratch)),
        out_shape=like + [home(w)((*dims, 2, *UNIT), bf16) for w in range(MATS)],
        in_specs=[vmem] * len(given),
        out_specs=[vmem] * len(like) + [anywhere] * MATS,
        scratch_shapes=list(scratch.values()),
        compiler_params=pltpu.CompilerParams(collective_id=2, has_side_effects=True, vmem_limit_bytes=VMEM_FEW),
        name="update",
    )(*given)
    return results[: len(like)], results[len(like) :]


VMEM_MOST, VMEM_SOME, VMEM_FEW = 62 << 20, 40 << 20, 12 << 20
VMEM_HALF = 20 << 20


def normed(h):
    wide = h.astype(f32)
    scale = lax.rsqrt(jnp.mean(wide**2, -1, keepdims=True) + 1e-6)
    return (wide * scale).astype(bf16)


def norm_back(h, da):
    wide, da = h.astype(f32), da.astype(f32)
    scale = lax.rsqrt(jnp.mean(wide**2, -1, keepdims=True) + 1e-6)
    inner = jnp.mean(wide * da, -1, keepdims=True)
    return (scale * da - wide * (inner * scale * scale * scale)).astype(bf16)


PLAIN, TURNED = ((1,), (0,)), ((1,), (1,))
ROWS = 128


def dot(a, b, dims):
    return lax.dot_general(a, b, (dims, ((), ())), preferred_element_type=f32)


def by_rows(ref, work):
    def some(i, _):
        work(pl.ds(pl.multiple_of(i * ROWS, ROWS), ROWS))
        return 0

    lax.fori_loop(0, ref.shape[0] // ROWS, some, 0)


def gate_back(dhid, gate, up):
    soft = jax.nn.sigmoid(gate)
    return dhid * up * (soft * (1.0 + gate * (1.0 - soft))), dhid * (gate * soft)


def bottom_kernel(h, wg, wu, wd, a, gate, up, hid, out, acc):
    step = pl.program_id(0)

    @pl.when(step == 0)
    def _():
        def first(rows):
            a[rows] = normed(h[rows])

        by_rows(h, first)

    for part in parts():
        gate[:, part] = dot(a[...], wg[0, :, part], PLAIN)
        up[:, part] = dot(a[...], wu[0, :, part], PLAIN)
        hid[:, part] = (jax.nn.silu(gate[:, part]) * up[:, part]).astype(bf16)
    term = dot(hid[...], wd[0], PLAIN)

    @pl.when(step == 0)
    def _():
        acc[...] = term

    @pl.when(step > 0)
    def _():
        acc[...] += term

    @pl.when(step == pl.num_programs(0) - 1)
    def _():
        def last(rows):
            out[rows] = h[rows] + acc[rows].astype(bf16)

        by_rows(h, last)


def top_kernel(h, dy, wg, wu, wd, a, hid, dgate, dup, dh, acc_gate, acc_up):
    step = pl.program_id(0)

    @pl.when(step == 0)
    def _():
        def first(rows):
            a[rows] = normed(h[rows])

        by_rows(h, first)

    for part in parts():
        gate = dot(a[...], wg[0, :, part], PLAIN)
        up = dot(a[...], wu[0, :, part], PLAIN)
        dhid = dot(dy[...], wd[0, part, :], TURNED).astype(bf16).astype(f32)
        hid[:, part] = (jax.nn.silu(gate) * up).astype(bf16)
        by_gate, by_up = gate_back(dhid, gate, up)
        dgate[:, part], dup[:, part] = by_gate.astype(bf16), by_up.astype(bf16)
    for acc, d, w in ((acc_gate, dgate, wg), (acc_up, dup, wu)):
        term = dot(d[...], w[0], TURNED)

        @pl.when(step == 0)
        def _():
            acc[...] = term

        @pl.when(step > 0)
        def _():
            acc[...] += term

    @pl.when(step == pl.num_programs(0) - 1)
    def _():
        def last(rows):
            da = acc_gate[rows].astype(bf16) + acc_up[rows].astype(bf16)
            dh[rows] = dy[rows] + norm_back(h[rows], da)

        by_rows(h, last)


def back_kernel(dh, gate, up, wd, dgate, dup):
    for part in parts():
        dhid = dot(dh[...], wd[0, part, :], TURNED).astype(bf16).astype(f32)
        by_gate, by_up = gate_back(dhid, gate[:, part], up[:, part])
        dgate[:, part], dup[:, part] = by_gate.astype(bf16), by_up.astype(bf16)


WIDTH, PART = 512, 256


def parts():
    return [slice(at, at + PART) for at in range(0, WIDTH, PART)]


def layer_call(kernel, layer, tokens_in, hidden_in, weights, hidden_out, tokens_out, accumulators, products, name):
    T, D = tokens_in[0].shape
    FF = weights[-1].shape[1]
    whole = pl.BlockSpec((T, D), lambda n: (0, 0))
    part = pl.BlockSpec((T, WIDTH), lambda n: (0, n))
    specs = [pl.BlockSpec((1, D, WIDTH), lambda n: (layer, 0, n))] * (len(weights) - 1) + [pl.BlockSpec((1, WIDTH, D), lambda n: (layer, n, 0))]
    early, late = tokens_out
    shape = jax.ShapeDtypeStruct
    return pl.pallas_call(
        kernel,
        grid=(FF // WIDTH,),
        in_specs=[whole] * len(tokens_in) + [part] * len(hidden_in) + specs,
        out_specs=[whole] * early + [part] * len(hidden_out) + [whole] * late,
        out_shape=[shape((T, D), bf16)] * early + [shape((T, FF), t) for t in hidden_out] + [shape((T, D), bf16)] * late,
        scratch_shapes=[pltpu.VMEM((T, D), f32)] * accumulators,
        cost_estimate=pl.CostEstimate(flops=2 * products * T * D * FF, bytes_accessed=2 * len(weights) * D * FF, transcendentals=T * FF),
        compiler_params=pltpu.CompilerParams(vmem_limit_bytes=VMEM_MOST),
        name=name,
    )(*tokens_in, *hidden_in, *weights)


def factors(x, dy, wg, wu, wd):
    weights = (wg, wu, wd)
    a0, gate, up, hid0, h = layer_call(bottom_kernel, 0, (x,), (), weights, (f32, f32, bf16), (1, 1), 1, 3, "bottom")
    a1, hid1, dg1, du1, dh = layer_call(top_kernel, 1, (h, dy), (), weights, (bf16,) * 3, (1, 1), 2, 5, "top")
    dg0, du0 = layer_call(back_kernel, 0, (dh,), (gate, up), (wd,), (bf16,) * 2, (0, 0), 0, 1, "back")
    return (hid1, dy), (a1, dg1), (a1, du1), (hid0, dh), (a0, dg0), (a0, du0)


def product_kernel(kind, left, right, *refs):
    out = refs[-1]
    C, width = SHAPES[kind][1], out.shape[5] * SHAPES[kind][1]
    for start in range(0, width, CHUNK):
        wide = lax.dot_general(left[...], right[:, start : start + CHUNK], (((0,), (0,)), ((), ())), preferred_element_type=f32)
        wide = wide.reshape(out.shape[2], out.shape[3], SHAPES[kind][0], CHUNK)
        if kind:
            for natural, unit in tiles(*DOWN):
                for core in range(out.shape[5]):
                    at = core * C + natural[1].start - start
                    if 0 <= at < CHUNK:
                        out[(0, 0, slice(None), slice(None), 0, core, *unit)] = wide[:, :, natural[0].start : natural[0].start + natural[0].size, at : at + natural[1].size].astype(bf16)
        else:
            for core in range(out.shape[5]):
                begin, end = max(start, core * C), min(start + CHUNK, core * C + C)
                if begin < end:
                    out[0, 0, :, :, 0, core, :, begin - core * C : end - core * C] = wide[..., begin - start : end - start].astype(bf16)


CHUNK = 256


def product(wave, left, right, into, dims):
    X, Y, Z = dims
    kind = WAVES[wave][0]
    R, C = SHAPES[kind]
    tokens, halves = right.shape[0], Z // 2
    given = [] if into is None else [into]
    return pl.pallas_call(
        functools.partial(product_kernel, kind),
        grid=(2, X),
        out_shape=jax.ShapeDtypeStruct((MATS, X, Y, halves, 2, 2, *UNIT), bf16),
        in_specs=[pl.BlockSpec((tokens, R * Y * halves), lambda p, i: (0, i)), pl.BlockSpec((tokens, 2 * C), lambda p, i: (0, p))]
        + [pl.BlockSpec(memory_space=pl.ANY)] * len(given),
        out_specs=pl.BlockSpec((1, 1, Y, halves, 1, 2, *UNIT), lambda p, i: (wave, i, 0, 0, p, 0, 0, 0)),
        input_output_aliases={2: 0} if given else {},
        cost_estimate=pl.CostEstimate(flops=2 * left.size * right.shape[1], bytes_accessed=2 * left.shape[1] * right.shape[1], transcendentals=0),
        compiler_params=pltpu.CompilerParams(vmem_limit_bytes=VMEM_MOST),
        name="product",
    )(left, right, *given)


SETTLED = (4, 1, 5, 2, 3, 0)
SHARE = 2


def settle_kernel(*refs):
    step = pl.program_id(0)
    for n, (wave, w) in enumerate(zip(SETTLED, refs)):
        kind, out = WAVES[wave][0], refs[MATS + n // 2]
        C = SHAPES[kind][1]

        @pl.when(step == n)
        def _():
            for q in range(4):
                block = w.at[0, :, :, q // 2, q % 2]
                if kind:
                    for natural, unit in tiles(*DOWN):
                        out[:, :, :, natural[0], pl.ds(C * q + natural[1].start, natural[1].size)] = block[(slice(None), slice(None), *unit)][None]
                else:
                    out[:, :, :, :, C * q : C * (q + 1)] = block[...][None]


def settle(waves, dims):
    X, Y, Z = dims
    X, Y, halves = X * SHARE, Y // SHARE, Z // 2
    shape = (Y, halves, 2, 2, *UNIT)

    def turn(first, last, n, i):
        return jnp.clip((n - first) * X + i, 0, (last - first + 1) * X - 1)

    def given(n):
        return pl.BlockSpec((1, *shape), lambda k, i: (turn(n, n, k, i), *[0] * len(shape)))

    def made(which):
        R, C = SHAPES[which // 2]

        def place(k, i):
            at = turn(2 * which, 2 * which + 1, k, i)
            return (at // X, at % X, 0, 0, 0)

        return pl.BlockSpec((1, Y, halves, R, 4 * C), place)

    outs = pl.pallas_call(
        settle_kernel,
        grid=(MATS, X),
        out_shape=[jax.ShapeDtypeStruct((2, X * Y, halves, SHAPES[which // 2][0], 4 * SHAPES[which // 2][1]), bf16) for which in range(3)],
        in_specs=[given(n) for n in range(MATS)],
        out_specs=[made(which) for which in range(3)],
        compiler_params=pltpu.CompilerParams(vmem_limit_bytes=VMEM_HALF),
        name="settle",
    )(*[pltpu.with_memory_space_constraint(waves[n].reshape(X, *shape), home(n)) for n in SETTLED])
    return [out.reshape(2, -1, out.shape[-1]) for out in outs]


def device_step(dims, x, dy, wg, wu, wd, *moments):
    m, v = moments[:3], moments[3:]
    g = None
    for wave, (left, right) in enumerate(factors(x[0], dy[0], wg, wu, wd)):
        g = product(wave, left, right, g, dims)
    grads = scatter(g.reshape(MATS, *dims, 2, *UNIT), dims)
    place = lax.axis_index("dp")
    w = [lax.dynamic_slice_in_dim(a, place * b.shape[1], b.shape[1], 1) for a, b in zip((wg, wu, wd), m, strict=True)]
    flip = [jnp.swapaxes(a, 0, 1) for a in (*m, *v)]
    mv, out = update(grads, w, flip, dims)
    mv = [jnp.swapaxes(a, 0, 1) for a in mv]
    return (*settle(out, dims), *mv)


DIMS = {256: (4, 4, 8)}


def solution(mesh):
    dims = DIMS[mesh.shape["dp"]]
    spec = jax.sharding.PartitionSpec
    tokens, whole, rows = spec(("rep", "dp")), spec(), spec(None, "dp", None)
    return jax.shard_map(
        functools.partial(device_step, dims),
        mesh=mesh,
        in_specs=(tokens, tokens, *[whole] * 3, *[rows] * 6),
        out_specs=(*[spec("rep")] * 3, *[spec("rep", "dp", None)] * 6),
        check_vma=False,
    )
```

```python
import functools
import jax, jax.numpy as jnp
from jax import lax
from jax.experimental import pallas as pl
from jax.experimental.pallas import tpu as pltpu

bf16, f32 = jnp.bfloat16, jnp.float32
MATS = 6
UNIT = (24, 896)
DOWN = (56, 384)
TILE = (8, 128)
PADS = (8, 16)
ORDERS = ("xyz", "yzx", "zxy")
COLUMNS = ((0, 384), (384, 256), (640, 256))
KINDS = ("s", "f", "z", "d", "e")
SCATTER_TIMES = '$*115::B$)-.24688;;A$()+//336<<A'
GATHER_TIMES, GATHER_STEPS = '#-.4799Yj~#337;<DEOPQ_oi#((3@AAKX\\bgoy', (4, 14)
MESH = pl.DeviceIdType.MESH
START, MORE = 0, 1
NORTH, SOUTH = 0, 1


def time_of(character):
    return ord(character) - ord("#")


class Torus:
    def __init__(self, dims):
        self.dims = dict(zip("xyz", dims))
        self.cores = 2
        _, Y, Z = dims
        self.stride = dict(zip("xyz", (Y * Z * self.cores, Z * self.cores, self.cores)))
        self.rep, self.idx = lax.axis_index("rep"), lax.axis_index("dp")
        self.at = {d: lax.rem(lax.div(self.idx, self.stride[d]), self.dims[d]) for d in "xyz"}
        self.core = lax.rem(self.idx, self.cores)

    def wrap(self, d, value):
        n = self.dims[d]
        return lax.rem(value + n, n)

    def beside(self, d, offset):
        return (self.rep, self.idx + (self.wrap(d, self.at[d] + offset) - self.at[d]) * self.stride[d])

    def partner(self):
        return (self.rep, self.idx + 1 - 2 * self.core)

    def everyone(self):
        return [self.beside(d, o) for d in "xyz" for o in range(1, self.dims[d])]

    def group(self, s):
        return (self.rep, self.idx - lax.rem(self.idx, 4) + s)

    def enter(self):
        me = lax.rem(self.idx, 4)
        barrier = pltpu.get_barrier_semaphore()
        devices = self.everyone() + [self.partner(), self.group(lax.rem(me + 3 - 2 * self.core, 4))]
        for device in devices:
            signal(barrier, device)
        pl.semaphore_wait(barrier, len(devices))


def signal(sem, device):
    pl.semaphore_signal(sem, inc=1, device_id=device, device_id_type=MESH)


def remote(src, dst, send, recv, device):
    return pltpu.make_async_remote_copy(src_ref=src, dst_ref=dst, send_sem=send, recv_sem=recv, device_id=device, device_id_type=MESH)


class Ring:
    def __init__(self, color, phase, d, n):
        self.name = f"{color.k}{phase}"
        self.color, self.phase, self.d, self.n = color, phase, d, n
        self.steps = (n // 2, (n - 1) // 2)
        self.sides = [side for side in (NORTH, SOUTH) if self.steps[side]]

    def message(self, side, m):
        return m + side * self.steps[NORTH]


class Color:
    def __init__(self, k, dims):
        self.k, self.order = k, ORDERS[k]
        start, self.width = COLUMNS[k]
        self.columns = pl.ds(start, self.width)
        size = dict(zip("xyz", dims))
        n = [size[d] for d in self.order]
        self.rings = [Ring(self, phase, d, m) for phase, (d, m) in enumerate(zip(self.order, n))]
        first, second, third = self.order
        self.rest = [d for d in "xyz" if d != first]
        self.block = (tuple(size[d] for d in self.rest), (size[third],))
        self.unit = (UNIT[0], self.width)

    def index(self, **at):
        return tuple(at.get(d, slice(None)) for d in "xyz")

    def within(self, b):
        return tuple(b if d == self.order[1] else slice(None) for d in self.rest)

    def events(self, gather):
        rings, direct = [], [("d", self, 2, START, START), ("e", self, 2, START, START)]
        for ring in self.rings[:2][:: -1 if gather else 1]:
            rings.append(("s", self, ring.phase, START, START))
            for j in range(1, ring.steps[NORTH] + gather):
                rings += [("f", self, ring.phase, side, j) for side in (NORTH, SOUTH) if side == NORTH or j < ring.steps[SOUTH] + gather]
            if not gather:
                rings.append(("z", self, ring.phase, START, START))
        return direct + rings if gather else rings + direct


def add_blocks(dst, dst_index, terms, shape):
    def at(ref, index, place):
        place = list(place)
        return ref[tuple([place.pop(0) if isinstance(e, slice) else e for e in index] + place)]

    def row(i, _):
        for rest in [(j,) for n in shape[1:] for j in range(n)] or [()]:
            place = (i, *rest)
            dst[(*dst_index, *place)] = sum(at(ref, index, place).astype(f32) for ref, index in terms).astype(dst.dtype)
        return 0

    lax.fori_loop(0, shape[0], row, 0)


def direct(t, ring, o, w, src, dst, s, slot, half):
    name = ring.name
    return remote(src, dst, s["send" + name].at[half, o - 1], s["recv" + name].at[slot, o - 1], t.beside(ring.d, o))


class Scatter:
    def __init__(self, dims):
        self.dims = dims
        self.X, self.Y, Z = dims
        self.halves = Z // 2
        self.tiles = 2 * self.X
        self.colors = [Color(k, dims) for k in range(len(ORDERS))]
        events = [e for c in self.colors for e in c.events(False)]
        lag = [divmod(time_of(c), self.tiles) for c in SCATTER_TIMES]
        self.order = [(e, *when) for e, when in zip(events, lag, strict=True)]
        self.lag = {e: when for e, *when in self.order}
        self.depth = max(lag for _, lag, _ in self.order)
        self.slots = self.depth + 1
        self.first = min((e for e in events if e[0] == "s" and not e[2]), key=lambda e: (*self.lag[e], events.index(e)))
        self.last = max((e for e in events if e[0] == "e"), key=lambda e: (*self.lag[e], events.index(e)))

    def scratch(self):
        shapes = {}
        NS = self.slots
        for c in self.colors:
            for ring in c.rings:
                n, name = ring.n, ring.name
                block = (c.block + ((),))[ring.phase] + c.unit
                shapes["recv" + name] = pltpu.SemaphoreType.DMA((NS, n - 1))
                shapes["send" + name] = pltpu.SemaphoreType.DMA((NS, n - 1))
                shapes["in" + name] = pltpu.VMEM((NS, n - 1) + block, bf16)
                shapes["out" + name] = pltpu.VMEM((self.kept(c, ring.phase, "s" if ring.phase < 2 else "d"), len(ring.sides) if ring.phase < 2 else n - 1) + block, bf16)
                if ring.phase < 2:
                    shapes["sum" + name] = pltpu.VMEM((self.kept(c, ring.phase, "z"),) + block, f32)
            n = c.rings[0].n
            shapes[f"load{c.k}"] = pltpu.VMEM((n, 2) + c.block[0] + c.unit, bf16)
            shapes[f"load_sem{c.k}"] = pltpu.SemaphoreType.DMA((n, 2))
        for name in ("part_send", "own", "left_sem", "right_sem"):
            shapes[name] = pltpu.SemaphoreType.DMA((2,))
        shapes["part_recv"] = pltpu.SemaphoreType.DMA((MATS,))
        shapes["left"] = pltpu.VMEM((2, self.tokens, self.Y * self.halves * DOWN[0]), bf16)
        shapes["right"] = pltpu.VMEM((2, self.tokens, 2 * UNIT[1]), bf16)
        shapes["stage"] = pltpu.VMEM((2, self.Y, self.halves, 2, *UNIT), bf16)
        shapes["free"] = pltpu.SemaphoreType.REGULAR((MATS,))
        return shapes

    def lags(self, c, phase, kinds):
        return [lag for e, lag, _ in self.order if e[1] is c and e[2] == phase and e[0] in kinds]

    def kept(self, c, phase, kind):
        if kind == "s":
            ends = self.lags(c, phase, "z")
        elif kind == "d":
            ends = self.lags(c, phase, "e")
        else:
            ends = self.lags(c, phase + 1, "ze")
        return max(ends) - min(self.lags(c, phase, kind)) + 1

    def bind(self, torus, lefts, rights, g, pg, unit, s):
        self.t, self.lefts, self.rights, self.g, self.pg, self.unit, self.s = torus, lefts, rights, g, pg, unit, s

    def spot(self, d, place):
        return lax.rem(place, 2) * self.halves + lax.div(place, 2) if d == "z" else place


    def left(self, m, x, slot):
        width = self.Y * self.halves * SHAPES[WAVES[m][0]][0]
        source = self.lefts[m].at[:, pl.ds(pl.multiple_of(x * width, width), width)]
        return pltpu.make_async_copy(source, self.s["left"].at[slot, :, pl.ds(0, width)], self.s["left_sem"].at[slot])

    def right(self, m, p):
        width = 2 * SHAPES[WAVES[m][0]][1]
        source = self.rights[m].at[:, pl.ds(p * width, width)]
        return pltpu.make_async_copy(source, self.s["right"].at[p, :, pl.ds(0, width)], self.s["right_sem"].at[p])

    def made(self, m, p, x, slot):
        t, s, stage = self.t, self.s, self.s["stage"]
        place = (m, x, slice(None), pl.ds(p * self.halves, self.halves))
        own = pltpu.make_async_copy(stage.at[slot, :, :, t.core], self.g.at[place], s["own"].at[slot])
        return own, remote(stage.at[slot, :, :, 1 - t.core], self.pg.at[place], s["part_send"].at[slot], s["part_recv"].at[m], t.partner())

    def settled(self, slot):
        own, theirs = self.made(0, 0, 0, slot)
        own.wait()
        theirs.wait_send()

    def multiply(self, kind, slot, p):
        R, C = SHAPES[kind]
        left, right, out = self.s["left"], self.s["right"], self.s["stage"]
        for start in range(0, 2 * C, CHUNK):
            wide = lax.dot_general(left[slot, :, 0 : self.Y * self.halves * R], right[p, :, start : start + CHUNK], (((0,), (0,)), ((), ())), preferred_element_type=f32)
            wide = wide.reshape(self.Y, self.halves, R, CHUNK)
            for core in range(2):
                if kind:
                    for natural, unit in tiles(*DOWN):
                        at = core * C + natural[1].start - start
                        if 0 <= at < CHUNK:
                            rows = slice(natural[0].start, natural[0].start + natural[0].size)
                            out[(slot, slice(None), slice(None), core, *unit)] = wide[:, :, rows, at : at + natural[1].size].astype(bf16)
                else:
                    begin, end = max(start, core * C), min(start + CHUNK, core * C + C)
                    if begin < end:
                        out[slot, :, :, core, :, begin - core * C : end - core * C] = wide[..., begin - start : end - start].astype(bf16)

    def tile(self, i, j):
        X = self.X
        slot, p, x = lax.rem(j, 2), lax.div(j, X), lax.rem(j, X)
        then = j + 1 == self.tiles
        following, beside = i + then.astype(jnp.int32), jnp.where(then, 0, j + 1)
        for m in range(MATS):

            @pl.when(following == m)
            def _():
                self.left(m, lax.rem(beside, X), lax.rem(beside, 2)).start()

            @pl.when((j == 0) & (i == m))
            def _():
                self.right(m, 1).start()

            @pl.when((j == X) & (i + 1 == m))
            def _():
                self.right(m, 0).start()

        @pl.when((j != 1) & (i + j > 0))
        def _():
            self.settled(slot)

        for m, kind in enumerate(k for k, _ in WAVES[:2]):

            @pl.when((lax.rem(i, 3) == 0) == (m == 0))
            def _():
                self.left(m, 0, slot).wait()

                @pl.when(x == 0)
                def _():
                    self.right(m, p).wait()

                self.multiply(kind, slot, p)

        for copy in self.made(i, p, x, slot):
            copy.start()

    def ready(self, w):
        self.settled(1)

        @pl.when(w == MATS - 1)
        def _():
            self.settled(0)

        s = self.s
        remote(self.pg.at[w], self.pg.at[w], s["part_send"].at[0], s["part_recv"].at[w], self.t.partner()).wait_recv()
        early, late = [], []
        for c in self.colors:
            ring = c.rings[0]
            for side in ring.sides:
                for j in range(ring.steps[side] + (side == NORTH)):
                    (late if self.consumer_lag(ring, side, j) else early).append((c, side, j))
        for c, side, j in early:
            self.start_loads(c, side, j, w)

        @pl.when(w == 0)
        def _():
            for c, side, j in late:
                self.start_loads(c, side, j, w)

    def consumer_lag(self, ring, side, j):
        c = ring.color
        if j == 0:
            e = ("s", c, 0, START, START)
        else:
            e = ("f", c, 0, side, j) if j < ring.steps[side] else ("z", c, 0, START, START)
        return self.lag[e][0]

    def start_loads(self, c, side, j, w):
        for copy in self.loads(c, side, j, w):
            copy.start()

    def sign(self, side, w):
        return (1 - 2 * lax.rem(w, 2)) * (1 - 2 * side)

    def target(self, ring, side, j, w):
        return self.t.wrap(ring.d, self.t.at[ring.d] + self.sign(side, w) * (ring.steps[side] - j))

    def loads(self, c, side, j, w):
        ring = c.rings[0]
        place = ring.message(side, j) if j < ring.steps[side] else ring.n - 1
        index = c.index(**{ring.d: self.spot(ring.d, self.target(ring, side, j, w))})
        columns = (slice(None), c.columns)
        buf, sem = self.s[f"load{c.k}"], self.s[f"load_sem{c.k}"]
        sources = self.g.at[(w, *index, *columns)], self.pg.at[(w, *index, *columns)]
        return [pltpu.make_async_copy(source, buf.at[place, n], sem.at[place, n]) for n, source in enumerate(sources)]

    def message(self, ring, side, m, w, src):
        s, name = self.s, ring.name
        n, slot = ring.message(side, m), lax.rem(w, self.slots)
        return remote(src, s["in" + name].at[slot, n], s["send" + name].at[slot, n], s["recv" + name].at[slot, n], self.t.beside(ring.d, self.sign(side, w)))

    def add(self, dst, index, ring, side, j, w, terms):
        c, s = ring.color, self.s
        if ring.phase:
            before = s["sum" + c.rings[0].name]
            own = [(before, (lax.rem(w, before.shape[0]), *c.within(self.spot(ring.d, self.target(ring, side, j, w)))))]
        else:
            place = ring.message(side, j) if j < ring.steps[side] else ring.n - 1
            for copy in self.loads(c, side, j, w):
                copy.wait()
            own = [(s[f"load{c.k}"], (place, n)) for n in range(2)]
        add_blocks(dst, index, own + terms, c.block[ring.phase])
        if not ring.phase and self.consumer_lag(ring, side, j):

            @pl.when(w + 1 < MATS)
            def _():
                self.start_loads(c, side, j, w + 1)

    def event(self, kind, c, phase, side, j, w):
        ring, s = c.rings[phase], self.s
        name, slot = ring.name, lax.rem(w, self.slots)
        box, out = s["in" + name], s["out" + name]
        part = lax.rem(w, out.shape[0])
        if kind == "s":
            for side in ring.sides:
                self.add(out, (part, side), ring, side, 0, w, [])
                self.message(ring, side, 0, w, out.at[part, side]).start()
        elif kind == "f":
            at = (slot, ring.message(side, j - 1))
            self.message(ring, side, j - 1, w, out.at[part, 0]).wait_recv()
            self.add(box, at, ring, side, j, w, [(box, at)])
            self.message(ring, side, j, w, box.at[at]).start()
        elif kind == "z":
            terms = []
            for side in ring.sides:
                m = ring.steps[side] - 1
                self.message(ring, side, m, w, out.at[part, 0]).wait_recv()
                terms.append((box, (slot, ring.message(side, m))))
            total = s["sum" + name]
            self.add(total, (lax.rem(w, total.shape[0]),), ring, NORTH, ring.steps[NORTH], w, terms)
            for side in ring.sides:
                for m in range(ring.steps[side]):
                    self.message(ring, side, m, w, out.at[part, 0]).wait_send()
        else:
            total = s["sum" + c.rings[1].name]
            last = lax.rem(w, total.shape[0])
            copies = [direct(self.t, ring, o, w, out.at[part, o - 1], box.at[slot, o - 1], s, slot, slot) for o in range(1, ring.n)]
            if kind == "d":
                for o, copy in enumerate(copies):
                    out[part, o] = total[last, self.spot(ring.d, self.t.wrap(ring.d, self.t.at[ring.d] + o + 1))].astype(bf16)
                    copy.start()
            else:
                value = total[last, self.spot(ring.d, self.t.at[ring.d])]
                for o, copy in enumerate(copies):
                    copy.wait_recv()
                    value = value + box[slot, o].astype(f32)
                self.unit[w, :, c.columns] = value
                for copy in copies:
                    copy.wait_send()

    def step(self, i, j):
        @pl.when(i < MATS)
        def _():
            self.tile(i, j)

        @pl.when((j == 0) & (i > 0) & (i <= MATS))
        def _():
            self.ready(i - 1)

        for at in range(self.tiles):

            @pl.when(j == at)
            def _():
                for e, lag, _ in sorted((n for n in self.order if n[2] == at), key=lambda n: n[1]):
                    self.turn(e, i - 1 - lag)

    def turn(self, e, w):
        @pl.when((w >= 0) & (w < MATS))
        def _():
            if e == self.first:

                @pl.when(w >= self.slots)
                def _():
                    pl.semaphore_wait(self.s["free"].at[w - self.slots], len(self.t.everyone()))

            self.event(*e, w)
            if e == self.last:

                @pl.when(w + self.slots < MATS)
                def _():
                    for device in self.t.everyone():
                        signal(self.s["free"].at[w], device)

    def run(self):
        self.left(0, 0, 0).start()
        self.right(0, 0).start()

        def body(n, _):
            self.step(lax.div(n, self.tiles), lax.rem(n, self.tiles))
            return 0

        lax.fori_loop(0, (MATS + self.slots) * self.tiles, body, 0)


CHUNK = 256
WAVES = ((1, 1), (0, 1), (0, 3), (1, 0), (0, 0), (0, 2))
SHAPES = (UNIT, DOWN)


def tiles(R, C):
    r, c = TILE
    across, wide = C // c, UNIT[1] // c
    for n in range(R * C // (r * c)):
        yield (pl.ds(n // across * r, r), pl.ds(n % across * c, c)), (pl.ds(n // wide * r, r), pl.ds(n % wide * c, c))


def exchange_scratch():
    shapes = {}
    for kind, (R, C) in enumerate(SHAPES):
        n = sum(w[0] == kind for w in WAVES)
        shapes[f"nat{kind}"] = pltpu.VMEM((R, C), f32)
        shapes[f"slab{kind}"] = pltpu.VMEM((4, n, PADS[kind], C), bf16)
        shapes[f"rows{kind}"] = pltpu.VMEM((4, n, PADS[kind], C), bf16)
    shapes["x_send"] = pltpu.SemaphoreType.DMA((2, 4))
    shapes["x_recv"] = pltpu.SemaphoreType.DMA((2, 4))
    return shapes


def exchange(t, s):
    me = lax.rem(t.idx, 4)
    copies = []
    for o in range(1, 4):
        to = lax.rem(me + o, 4)
        for kind in range(2):
            copies.append(remote(s[f"slab{kind}"].at[to], s[f"rows{kind}"].at[me], s["x_send"].at[kind, o], s["x_recv"].at[kind, o], t.group(to)))
    for copy in copies:
        copy.start()
    for kind in range(2):
        s[f"rows{kind}"][me] = s[f"slab{kind}"][me]
    for copy in copies:
        copy.wait()


def scatter_kernel(dims, names, *refs):
    take = iter(refs)
    lefts, rights, outs = ([next(take) for _ in range(n)] for n in (MATS, MATS, 2))
    g, pg = next(take), next(take)
    s = dict(zip(names, take, strict=True))
    t = Torus(dims)
    t.enter()
    sc = Scatter(dims)
    sc.bind(t, lefts, rights, g, pg, s["unit"], s)
    sc.run()
    for w, (kind, at) in enumerate(WAVES):
        R, C = SHAPES[kind]
        nat, slab = s[f"nat{kind}"], s[f"slab{kind}"]
        for natural, unit in tiles(R, C):
            nat[natural] = s["unit"][(w, *unit)]
        rows = R // 4
        for q in range(4):
            slab[q, at, 0:rows, :] = nat[q * rows : (q + 1) * rows, :].astype(bf16)
    exchange(t, s)
    for kind, out in enumerate(outs):
        C = SHAPES[kind][1]
        for q in range(4):
            out[:, :, C * q : C * (q + 1)] = s[f"rows{kind}"][q]


def places():
    return pl.BlockSpec(memory_space=pl.ANY), pl.BlockSpec(memory_space=pltpu.VMEM)


def scatter(factors, dims):
    sc = Scatter(dims)
    sc.tokens = factors[0][0].shape[0]
    scratch = sc.scratch() | {"unit": pltpu.VMEM((MATS, *UNIT), f32)} | exchange_scratch()
    anywhere, vmem = places()
    rows = [jax.ShapeDtypeStruct((sum(w[0] == kind for w in WAVES), PADS[kind], 4 * C), bf16) for kind, (_, C) in enumerate(SHAPES)]
    terms = jax.ShapeDtypeStruct((MATS, *dims, *UNIT), bf16)
    *grads, _, _ = pl.pallas_call(
        functools.partial(scatter_kernel, dims, tuple(scratch)),
        out_shape=(*rows, terms, terms),
        in_specs=[anywhere] * 2 * MATS,
        out_specs=(vmem, vmem, anywhere, anywhere),
        scratch_shapes=list(scratch.values()),
        compiler_params=pltpu.CompilerParams(collective_id=1, has_side_effects=True, vmem_limit_bytes=VMEM_MOST),
        name="scatter",
    )(*[left for left, _ in factors], *[right for _, right in factors])
    return grads


class Gather:
    def __init__(self, dims):
        self.colors = [Color(k, dims) for k in range(len(ORDERS))]
        events = [e for c in self.colors for e in c.events(True)]
        timed = []
        for n, (e, character) in enumerate(zip(events, GATHER_TIMES, strict=True)):
            for w in range(MATS):
                timed.append((time_of(character) + GATHER_STEPS[e[2] == START] * w, w, n))
        self.order = [(events[n], w) for _, w, n in sorted(timed)]

    def scratch(self):
        shapes = {}
        for c in self.colors:
            for ring in c.rings:
                for way in ("send", "recv"):
                    shapes[way + ring.name] = pltpu.SemaphoreType.DMA((MATS, ring.n - 1))
        for name in ("over_send", "over_recv"):
            shapes[name] = pltpu.SemaphoreType.DMA((MATS, len(ORDERS)))
        shapes["own"] = pltpu.SemaphoreType.DMA((MATS,))
        return shapes

    def bind(self, torus, out, unit, s):
        self.t, self.out, self.unit, self.s = torus, out, unit, s

    def place(self, c, w, core, **at):
        return self.out[w].at[(*c.index(**at), core, slice(None), c.columns)]

    def own(self, w):
        t = self.t
        return pltpu.make_async_copy(self.unit.at[w], self.out[w].at[(*t.at.values(), t.core)], self.s["own"].at[w])

    def directs(self, ring, w):
        c, t = ring.color, self.t
        src, dst = self.unit.at[w, :, c.columns], self.place(c, w, t.core, **t.at)
        return [direct(t, ring, o, w, src, dst, self.s, w, w) for o in range(1, ring.n)]

    def message(self, ring, side, m, w):
        t, c, s = self.t, ring.color, self.s
        sign = (1 - 2 * side) * (1 - 2 * (w % 2))
        at = {d: t.at[d] for d in c.order[: ring.phase]} | {ring.d: t.wrap(ring.d, t.at[ring.d] - sign * m)}
        block, n = self.place(c, w, t.core, **at), ring.message(side, m)
        return remote(block, block, s["send" + ring.name].at[w, n], s["recv" + ring.name].at[w, n], t.beside(ring.d, sign))

    def over(self, c, w, core, **at):
        block = self.place(c, w, core, **at)
        return remote(block, block, self.s["over_send"].at[w, c.k], self.s["over_recv"].at[w, c.k], self.t.partner())

    def event(self, kind, c, phase, side, j, w):
        ring, t = c.rings[phase], self.t
        if kind == "d":
            for copy in self.directs(ring, w):
                copy.start()
        elif kind == "e":
            for copy in self.directs(ring, w):
                copy.wait_recv()
        elif kind == "s":
            for side in ring.sides:
                self.message(ring, side, 0, w).start()
            if not phase:
                self.over(c, w, t.core, **{ring.d: t.at[ring.d]}).start()
        else:
            self.message(ring, side, j - 1, w).wait_recv()
            if j < ring.steps[side]:
                self.message(ring, side, j, w).start()
            if not phase:
                sign = (1 - 2 * side) * (1 - 2 * (w % 2))
                self.over(c, w, t.core, **{ring.d: t.wrap(ring.d, t.at[ring.d] - sign * j)}).start()

    def finish(self, w):
        for c in self.colors:
            for ring in c.rings:
                if ring.phase == 2:
                    for copy in self.directs(ring, w):
                        copy.wait_send()
                else:
                    for side in ring.sides:
                        for m in range(ring.steps[side]):
                            self.message(ring, side, m, w).wait_send()
            self.over(c, w, self.t.core).wait_send()
            self.over(c, w, 1 - self.t.core).wait_recv()

    def run(self):
        for w in range(MATS):
            self.own(w).wait()
        for e, w in self.order:
            self.event(*e, w)
        for w in range(MATS):
            self.finish(w)


AXES = ("core", "x", "y", "z")


def sum_over_all(t, s, value):
    for n, d in enumerate(AXES):
        mine, box = s["norm_out"].at[n], s["norm_" + d]
        mine[...] = value
        copies = []
        for o in range(box.shape[0]):
            device = t.partner() if d == "core" else t.beside(d, o + 1)
            copies.append(remote(mine, box.at[o], s["norm_send"].at[n, o], s["norm_recv"].at[n, o], device))
        for copy in copies:
            copy.start()
        for copy in copies:
            copy.wait()
        for o in range(box.shape[0]):
            value = value + box[o]
    return value


def update_kernel(dims, names, *refs):
    take = iter(refs)
    grads, w_in, m_in, v_in, m_out, v_out = ([next(take) for _ in range(n)] for n in (2, 3, 3, 3, 3, 3))
    out = [next(take) for _ in WAVES]
    s = dict(zip(names, take, strict=True))
    t = Torus(dims)
    t.enter()

    def rows(kind, at):
        return grads[kind][at, 0 : SHAPES[kind][0] // 4, :].astype(f32)

    total, count = jnp.zeros((1, 1), f32), 0
    for kind, at in WAVES:
        g = rows(kind, at)
        count += g.size
        total = total + jnp.sum(jnp.sum(g * g, axis=0, keepdims=True), axis=1, keepdims=True)
    for d in AXES:
        count *= s["norm_" + d].shape[0] + 1
    total = sum_over_all(t, s, jnp.broadcast_to(total, TILE))[0:1, 0:1]
    factor = jnp.minimum(1.0, 0.5 * lax.rsqrt(total / count + 1e-30))

    for kind, at in WAVES:
        which, layer = (2, at) if kind else divmod(at, 2)
        R, C = SHAPES[kind]
        g = rows(kind, at) * factor
        w = w_in[which][layer].astype(f32)
        m = 0.9 * m_in[which][:, layer, :] + 0.1 * g
        v = 0.95 * v_in[which][:, layer, :] + 0.05 * g * g
        m_out[which][:, layer, :] = m
        v_out[which][:, layer, :] = v
        w = (w - 0.02 * (m * lax.rsqrt(v + 1e-8) + 0.1 * w)).astype(bf16)
        for q in range(4):
            s[f"slab{kind}"][q, at, 0 : R // 4, :] = w[:, C * q : C * (q + 1)]
    exchange(t, s)
    ga = Gather(dims)
    ga.bind(t, out, s["unit"], s)
    for w, (kind, at) in enumerate(WAVES):
        R, C = SHAPES[kind]
        nat, rows_in, n = s[f"nat{kind}"], s[f"rows{kind}"], R // 4
        for q in range(4):
            nat[q * n : (q + 1) * n, :] = rows_in[q, at, 0:n, :].astype(f32)
        for natural, unit in tiles(R, C):
            s["wide"][unit] = nat[natural]
        s["unit"][w] = s["wide"][...].astype(bf16)
        ga.own(w).start()
    ga.run()


IN_VMEM = (1, 2, 4)


def home(wave):
    return pltpu.VMEM if wave in IN_VMEM else pltpu.HBM


def update(grads, w, moments, dims):
    scratch = Gather(dims).scratch() | exchange_scratch()
    scratch["unit"] = pltpu.VMEM((MATS, *UNIT), bf16)
    scratch["wide"] = pltpu.VMEM(UNIT, f32)
    scratch["norm_out"] = pltpu.VMEM((len(AXES), *TILE), f32)
    for d, n in zip(AXES, (2, *dims), strict=True):
        scratch["norm_" + d] = pltpu.VMEM((n - 1, *TILE), f32)
    for name in ("norm_send", "norm_recv"):
        scratch[name] = pltpu.SemaphoreType.DMA((len(AXES), max(dims)))
    anywhere, vmem = places()
    given = (*grads, *w, *moments)
    like = [jax.ShapeDtypeStruct(a.shape, f32) for a in moments]
    results = pl.pallas_call(
        functools.partial(update_kernel, dims, tuple(scratch)),
        out_shape=like + [home(w)((*dims, 2, *UNIT), bf16) for w in range(MATS)],
        in_specs=[vmem] * len(given),
        out_specs=[vmem] * len(like) + [anywhere] * MATS,
        scratch_shapes=list(scratch.values()),
        compiler_params=pltpu.CompilerParams(collective_id=2, has_side_effects=True, vmem_limit_bytes=VMEM_FEW),
        name="update",
    )(*given)
    return results[: len(like)], results[len(like) :]


VMEM_MOST, VMEM_SOME, VMEM_FEW = 62 << 20, 40 << 20, 12 << 20
VMEM_HALF = 20 << 20


def normed(h):
    wide = h.astype(f32)
    scale = lax.rsqrt(jnp.mean(wide**2, -1, keepdims=True) + 1e-6)
    return (wide * scale).astype(bf16)


def norm_back(h, da):
    wide, da = h.astype(f32), da.astype(f32)
    scale = lax.rsqrt(jnp.mean(wide**2, -1, keepdims=True) + 1e-6)
    inner = jnp.mean(wide * da, -1, keepdims=True)
    return (scale * da - wide * (inner * scale * scale * scale)).astype(bf16)


PLAIN, TURNED = ((1,), (0,)), ((1,), (1,))
ROWS = 128


def dot(a, b, dims):
    return lax.dot_general(a, b, (dims, ((), ())), preferred_element_type=f32)


def by_rows(ref, work):
    def some(i, _):
        work(pl.ds(pl.multiple_of(i * ROWS, ROWS), ROWS))
        return 0

    lax.fori_loop(0, ref.shape[0] // ROWS, some, 0)


def gate_back(dhid, gate, up):
    soft = jax.nn.sigmoid(gate)
    return dhid * up * (soft * (1.0 + gate * (1.0 - soft))), dhid * (gate * soft)


def bottom_kernel(h, wg, wu, wd, a, gate, up, hid, out, acc):
    step = pl.program_id(0)

    @pl.when(step == 0)
    def _():
        def first(rows):
            a[rows] = normed(h[rows])

        by_rows(h, first)

    for part in parts():
        gate[:, part] = dot(a[...], wg[0, :, part], PLAIN)
        up[:, part] = dot(a[...], wu[0, :, part], PLAIN)
        hid[:, part] = (jax.nn.silu(gate[:, part]) * up[:, part]).astype(bf16)
    term = dot(hid[...], wd[0], PLAIN)

    @pl.when(step == 0)
    def _():
        acc[...] = term

    @pl.when(step > 0)
    def _():
        acc[...] += term

    @pl.when(step == pl.num_programs(0) - 1)
    def _():
        def last(rows):
            out[rows] = h[rows] + acc[rows].astype(bf16)

        by_rows(h, last)


def top_kernel(h, dy, wg, wu, wd, a, hid, dgate, dup, dh, acc_gate, acc_up):
    step = pl.program_id(0)

    @pl.when(step == 0)
    def _():
        def first(rows):
            a[rows] = normed(h[rows])

        by_rows(h, first)

    for part in parts():
        gate = dot(a[...], wg[0, :, part], PLAIN)
        up = dot(a[...], wu[0, :, part], PLAIN)
        dhid = dot(dy[...], wd[0, part, :], TURNED).astype(bf16).astype(f32)
        hid[:, part] = (jax.nn.silu(gate) * up).astype(bf16)
        by_gate, by_up = gate_back(dhid, gate, up)
        dgate[:, part], dup[:, part] = by_gate.astype(bf16), by_up.astype(bf16)
    for acc, d, w in ((acc_gate, dgate, wg), (acc_up, dup, wu)):
        term = dot(d[...], w[0], TURNED)

        @pl.when(step == 0)
        def _():
            acc[...] = term

        @pl.when(step > 0)
        def _():
            acc[...] += term

    @pl.when(step == pl.num_programs(0) - 1)
    def _():
        def last(rows):
            da = acc_gate[rows].astype(bf16) + acc_up[rows].astype(bf16)
            dh[rows] = dy[rows] + norm_back(h[rows], da)

        by_rows(h, last)


def back_kernel(dh, gate, up, wd, dgate, dup):
    for part in parts():
        dhid = dot(dh[...], wd[0, part, :], TURNED).astype(bf16).astype(f32)
        by_gate, by_up = gate_back(dhid, gate[:, part], up[:, part])
        dgate[:, part], dup[:, part] = by_gate.astype(bf16), by_up.astype(bf16)


WIDTH, PART = 512, 256


def parts():
    return [slice(at, at + PART) for at in range(0, WIDTH, PART)]


def layer_call(kernel, layer, tokens_in, hidden_in, weights, hidden_out, tokens_out, accumulators, products, name):
    T, D = tokens_in[0].shape
    FF = weights[-1].shape[1]
    whole = pl.BlockSpec((T, D), lambda n: (0, 0))
    part = pl.BlockSpec((T, WIDTH), lambda n: (0, n))
    specs = [pl.BlockSpec((1, D, WIDTH), lambda n: (layer, 0, n))] * (len(weights) - 1) + [pl.BlockSpec((1, WIDTH, D), lambda n: (layer, n, 0))]
    early, late = tokens_out
    shape = jax.ShapeDtypeStruct
    return pl.pallas_call(
        kernel,
        grid=(FF // WIDTH,),
        in_specs=[whole] * len(tokens_in) + [part] * len(hidden_in) + specs,
        out_specs=[whole] * early + [part] * len(hidden_out) + [whole] * late,
        out_shape=[shape((T, D), bf16)] * early + [shape((T, FF), t) for t in hidden_out] + [shape((T, D), bf16)] * late,
        scratch_shapes=[pltpu.VMEM((T, D), f32)] * accumulators,
        cost_estimate=pl.CostEstimate(flops=2 * products * T * D * FF, bytes_accessed=2 * len(weights) * D * FF, transcendentals=T * FF),
        compiler_params=pltpu.CompilerParams(vmem_limit_bytes=VMEM_MOST),
        name=name,
    )(*tokens_in, *hidden_in, *weights)


def factors(x, dy, wg, wu, wd):
    weights = (wg, wu, wd)
    a0, gate, up, hid0, h = layer_call(bottom_kernel, 0, (x,), (), weights, (f32, f32, bf16), (1, 1), 1, 3, "bottom")
    a1, hid1, dg1, du1, dh = layer_call(top_kernel, 1, (h, dy), (), weights, (bf16,) * 3, (1, 1), 2, 5, "top")
    dg0, du0 = layer_call(back_kernel, 0, (dh,), (gate, up), (wd,), (bf16,) * 2, (0, 0), 0, 1, "back")
    return (hid1, dy), (a1, dg1), (a1, du1), (hid0, dh), (a0, dg0), (a0, du0)


SETTLED = (4, 1, 5, 2, 3, 0)
SHARE = 2


def settle_kernel(*refs):
    step = pl.program_id(0)
    for n, (wave, w) in enumerate(zip(SETTLED, refs)):
        kind, out = WAVES[wave][0], refs[MATS + n // 2]
        C = SHAPES[kind][1]

        @pl.when(step == n)
        def _():
            for q in range(4):
                block = w.at[0, :, :, q // 2, q % 2]
                if kind:
                    for natural, unit in tiles(*DOWN):
                        out[:, :, :, natural[0], pl.ds(C * q + natural[1].start, natural[1].size)] = block[(slice(None), slice(None), *unit)][None]
                else:
                    out[:, :, :, :, C * q : C * (q + 1)] = block[...][None]


def settle(waves, dims):
    X, Y, Z = dims
    X, Y, halves = X * SHARE, Y // SHARE, Z // 2
    shape = (Y, halves, 2, 2, *UNIT)

    def turn(first, last, n, i):
        return jnp.clip((n - first) * X + i, 0, (last - first + 1) * X - 1)

    def given(n):
        return pl.BlockSpec((1, *shape), lambda k, i: (turn(n, n, k, i), *[0] * len(shape)))

    def made(which):
        R, C = SHAPES[which // 2]

        def place(k, i):
            at = turn(2 * which, 2 * which + 1, k, i)
            return (at // X, at % X, 0, 0, 0)

        return pl.BlockSpec((1, Y, halves, R, 4 * C), place)

    outs = pl.pallas_call(
        settle_kernel,
        grid=(MATS, X),
        out_shape=[jax.ShapeDtypeStruct((2, X * Y, halves, SHAPES[which // 2][0], 4 * SHAPES[which // 2][1]), bf16) for which in range(3)],
        in_specs=[given(n) for n in range(MATS)],
        out_specs=[made(which) for which in range(3)],
        compiler_params=pltpu.CompilerParams(vmem_limit_bytes=VMEM_HALF),
        name="settle",
    )(*[pltpu.with_memory_space_constraint(waves[n].reshape(X, *shape), home(n)) for n in SETTLED])
    return [out.reshape(2, -1, out.shape[-1]) for out in outs]


def device_step(dims, x, dy, wg, wu, wd, *moments):
    m, v = moments[:3], moments[3:]
    grads = scatter(factors(x[0], dy[0], wg, wu, wd), dims)
    place = lax.axis_index("dp")
    w = [lax.dynamic_slice_in_dim(a, place * b.shape[1], b.shape[1], 1) for a, b in zip((wg, wu, wd), m, strict=True)]
    flip = [jnp.swapaxes(a, 0, 1) for a in (*m, *v)]
    mv, out = update(grads, w, flip, dims)
    mv = [jnp.swapaxes(a, 0, 1) for a in mv]
    return (*settle(out, dims), *mv)


DIMS = {256: (4, 4, 8)}


def solution(mesh):
    dims = DIMS[mesh.shape["dp"]]
    spec = jax.sharding.PartitionSpec
    tokens, whole, rows = spec(("rep", "dp")), spec(), spec(None, "dp", None)
    return jax.shard_map(
        functools.partial(device_step, dims),
        mesh=mesh,
        in_specs=(tokens, tokens, *[whole] * 3, *[rows] * 6),
        out_specs=(*[spec("rep")] * 3, *[spec("rep", "dp", None)] * 6),
        check_vma=False,
    )
```

```python
import functools
import jax, jax.numpy as jnp
from jax import lax
from jax.experimental import pallas as pl
from jax.experimental.pallas import tpu as pltpu

bf16, f32 = jnp.bfloat16, jnp.float32
MATS = 6
UNIT = (24, 896)
DOWN = (56, 384)
TILE = (8, 128)
PADS = (8, 16)
ORDERS = ("xyz", "yzx", "zxy")
COLUMNS = ((0, 384), (384, 256), (640, 256))
KINDS = ("s", "f", "z", "d", "e")
SCATTER_TIMES = '$*115::B$)-.24688;;A$()+//336<<A'
GATHER_TIMES, GATHER_STEPS = '#-.4799Yj~#337;<DEOPQ_oi#((3@AAKX\\bgoy', (4, 14)
MESH = pl.DeviceIdType.MESH
START, MORE = 0, 1
NORTH, SOUTH = 0, 1


def time_of(character):
    return ord(character) - ord("#")


class Torus:
    def __init__(self, dims):
        self.dims = dict(zip("xyz", dims))
        self.cores = 2
        _, Y, Z = dims
        self.stride = dict(zip("xyz", (Y * Z * self.cores, Z * self.cores, self.cores)))
        self.rep, self.idx = lax.axis_index("rep"), lax.axis_index("dp")
        self.at = {d: lax.rem(lax.div(self.idx, self.stride[d]), self.dims[d]) for d in "xyz"}
        self.core = lax.rem(self.idx, self.cores)

    def wrap(self, d, value):
        n = self.dims[d]
        return lax.rem(value + n, n)

    def beside(self, d, offset):
        return (self.rep, self.idx + (self.wrap(d, self.at[d] + offset) - self.at[d]) * self.stride[d])

    def partner(self):
        return (self.rep, self.idx + 1 - 2 * self.core)

    def everyone(self):
        return [self.beside(d, o) for d in "xyz" for o in range(1, self.dims[d])]

    def group(self, s):
        return (self.rep, self.idx - lax.rem(self.idx, 4) + s)

    def crossed(self):
        return self.group(lax.rem(lax.rem(self.idx, 4) + 3 - 2 * self.core, 4))


def enter(devices):
    barrier = pltpu.get_barrier_semaphore()
    for device in devices:
        signal(barrier, device)
    pl.semaphore_wait(barrier, len(devices))


def signal(sem, device):
    pl.semaphore_signal(sem, inc=1, device_id=device, device_id_type=MESH)


def remote(src, dst, send, recv, device):
    return pltpu.make_async_remote_copy(src_ref=src, dst_ref=dst, send_sem=send, recv_sem=recv, device_id=device, device_id_type=MESH)


class Ring:
    def __init__(self, color, phase, d, n):
        self.name = f"{color.k}{phase}"
        self.color, self.phase, self.d, self.n = color, phase, d, n
        self.steps = (n // 2, (n - 1) // 2)
        self.sides = [side for side in (NORTH, SOUTH) if self.steps[side]]

    def message(self, side, m):
        return m + side * self.steps[NORTH]


class Color:
    def __init__(self, k, dims):
        self.k, self.order = k, ORDERS[k]
        start, self.width = COLUMNS[k]
        self.columns = pl.ds(start, self.width)
        size = dict(zip("xyz", dims))
        n = [size[d] for d in self.order]
        self.rings = [Ring(self, phase, d, m) for phase, (d, m) in enumerate(zip(self.order, n))]
        first, second, third = self.order
        self.rest = [d for d in "xyz" if d != first]
        self.block = (tuple(size[d] for d in self.rest), (size[third],))
        self.unit = (UNIT[0], self.width)

    def index(self, **at):
        return tuple(at.get(d, slice(None)) for d in "xyz")

    def within(self, b):
        return tuple(b if d == self.order[1] else slice(None) for d in self.rest)

    def events(self, gather):
        rings, direct = [], [("d", self, 2, START, START), ("e", self, 2, START, START)]
        for ring in self.rings[:2][:: -1 if gather else 1]:
            rings.append(("s", self, ring.phase, START, START))
            for j in range(1, ring.steps[NORTH] + gather):
                rings += [("f", self, ring.phase, side, j) for side in (NORTH, SOUTH) if side == NORTH or j < ring.steps[SOUTH] + gather]
            if not gather:
                rings.append(("z", self, ring.phase, START, START))
        return direct + rings if gather else rings + direct


def add_blocks(dst, dst_index, terms, shape):
    def at(ref, index, place):
        place = list(place)
        return ref[tuple([place.pop(0) if isinstance(e, slice) else e for e in index] + place)]

    def row(i, _):
        for rest in [(j,) for n in shape[1:] for j in range(n)] or [()]:
            place = (i, *rest)
            dst[(*dst_index, *place)] = sum(at(ref, index, place).astype(f32) for ref, index in terms).astype(dst.dtype)
        return 0

    lax.fori_loop(0, shape[0], row, 0)


def direct(t, ring, o, w, src, dst, s, slot, half):
    name = ring.name
    return remote(src, dst, s["send" + name].at[half, o - 1], s["recv" + name].at[slot, o - 1], t.beside(ring.d, o))


class Scatter:
    def __init__(self, dims):
        self.dims = dims
        self.X, self.Y, Z = dims
        self.halves = Z // 2
        self.tiles = 2 * self.X
        self.colors = [Color(k, dims) for k in range(len(ORDERS))]
        events = [e for c in self.colors for e in c.events(False)]
        lag = [divmod(time_of(c), self.tiles) for c in SCATTER_TIMES]
        self.order = [(e, *when) for e, when in zip(events, lag, strict=True)]
        self.lag = {e: when for e, *when in self.order}
        self.depth = max(lag for _, lag, _ in self.order)
        self.slots = self.depth + 1
        self.first = min((e for e in events if e[0] == "s" and not e[2]), key=lambda e: (*self.lag[e], events.index(e)))
        self.last = max((e for e in events if e[0] == "e"), key=lambda e: (*self.lag[e], events.index(e)))

    def scratch(self):
        shapes = {}
        NS = self.slots
        for c in self.colors:
            for ring in c.rings:
                n, name = ring.n, ring.name
                block = (c.block + ((),))[ring.phase] + c.unit
                shapes["recv" + name] = pltpu.SemaphoreType.DMA((NS, n - 1))
                shapes["send" + name] = pltpu.SemaphoreType.DMA((NS, n - 1))
                shapes["in" + name] = pltpu.VMEM((NS, n - 1) + block, bf16)
                shapes["out" + name] = pltpu.VMEM((self.kept(c, ring.phase, "s" if ring.phase < 2 else "d"), len(ring.sides) if ring.phase < 2 else n - 1) + block, bf16)
                if ring.phase < 2:
                    shapes["sum" + name] = pltpu.VMEM((self.kept(c, ring.phase, "z"),) + block, f32)
            n = c.rings[0].n
            shapes[f"load{c.k}"] = pltpu.VMEM((n, 2) + c.block[0] + c.unit, bf16)
            shapes[f"load_sem{c.k}"] = pltpu.SemaphoreType.DMA((n, 2))
        for name in ("part_send", "own", "left_sem", "right_sem"):
            shapes[name] = pltpu.SemaphoreType.DMA((2,))
        shapes["part_recv"] = pltpu.SemaphoreType.DMA((MATS,))
        shapes["left"] = pltpu.VMEM((2, self.tokens, self.Y * self.halves * DOWN[0]), bf16)
        shapes["right"] = pltpu.VMEM((2, self.tokens, 2 * UNIT[1]), bf16)
        shapes["stage"] = pltpu.VMEM((2, self.Y, self.halves, 2, *UNIT), bf16)
        shapes["free"] = pltpu.SemaphoreType.REGULAR((MATS,))
        return shapes

    def lags(self, c, phase, kinds):
        return [lag for e, lag, _ in self.order if e[1] is c and e[2] == phase and e[0] in kinds]

    def kept(self, c, phase, kind):
        if kind == "s":
            ends = self.lags(c, phase, "z")
        elif kind == "d":
            ends = self.lags(c, phase, "e")
        else:
            ends = self.lags(c, phase + 1, "ze")
        return max(ends) - min(self.lags(c, phase, kind)) + 1

    def bind(self, torus, lefts, rights, g, pg, unit, s):
        self.t, self.lefts, self.rights, self.g, self.pg, self.unit, self.s = torus, lefts, rights, g, pg, unit, s

    def spot(self, d, place):
        return lax.rem(place, 2) * self.halves + lax.div(place, 2) if d == "z" else place


    def left(self, m, x, slot):
        width = self.Y * self.halves * SHAPES[WAVES[m][0]][0]
        source = self.lefts[m].at[:, pl.ds(pl.multiple_of(x * width, width), width)]
        return pltpu.make_async_copy(source, self.s["left"].at[slot, :, pl.ds(0, width)], self.s["left_sem"].at[slot])

    def right(self, m, p):
        width = 2 * SHAPES[WAVES[m][0]][1]
        source = self.rights[m].at[:, pl.ds(p * width, width)]
        return pltpu.make_async_copy(source, self.s["right"].at[p, :, pl.ds(0, width)], self.s["right_sem"].at[p])

    def made(self, m, p, x, slot):
        t, s, stage = self.t, self.s, self.s["stage"]
        place = (m, x, slice(None), pl.ds(p * self.halves, self.halves))
        own = pltpu.make_async_copy(stage.at[slot, :, :, t.core], self.g.at[place], s["own"].at[slot])
        return own, remote(stage.at[slot, :, :, 1 - t.core], self.pg.at[place], s["part_send"].at[slot], s["part_recv"].at[m], t.partner())

    def settled(self, slot):
        own, theirs = self.made(0, 0, 0, slot)
        own.wait()
        theirs.wait_send()

    def multiply(self, kind, slot, p):
        R, C = SHAPES[kind]
        left, right, out = self.s["left"], self.s["right"], self.s["stage"]
        for start in range(0, 2 * C, CHUNK):
            wide = lax.dot_general(left[slot, :, 0 : self.Y * self.halves * R], right[p, :, start : start + CHUNK], (((0,), (0,)), ((), ())), preferred_element_type=f32)
            wide = wide.reshape(self.Y, self.halves, R, CHUNK)
            for core in range(2):
                if kind:
                    for natural, unit in tiles(*DOWN):
                        at = core * C + natural[1].start - start
                        if 0 <= at < CHUNK:
                            rows = slice(natural[0].start, natural[0].start + natural[0].size)
                            out[(slot, slice(None), slice(None), core, *unit)] = wide[:, :, rows, at : at + natural[1].size].astype(bf16)
                else:
                    begin, end = max(start, core * C), min(start + CHUNK, core * C + C)
                    if begin < end:
                        out[slot, :, :, core, :, begin - core * C : end - core * C] = wide[..., begin - start : end - start].astype(bf16)

    def tile(self, i, j):
        X = self.X
        slot, p, x = lax.rem(j, 2), lax.div(j, X), lax.rem(j, X)
        then = j + 1 == self.tiles
        following, beside = i + then.astype(jnp.int32), jnp.where(then, 0, j + 1)
        for m in range(MATS):

            @pl.when(following == m)
            def _():
                self.left(m, lax.rem(beside, X), lax.rem(beside, 2)).start()

            @pl.when((j == 0) & (i == m))
            def _():
                self.right(m, 1).start()

            @pl.when((j == X) & (i + 1 == m))
            def _():
                self.right(m, 0).start()

        @pl.when((j != 1) & (i + j > 0))
        def _():
            self.settled(slot)

        for m, kind in enumerate(k for k, _ in WAVES[:2]):

            @pl.when((lax.rem(i, 3) == 0) == (m == 0))
            def _():
                self.left(m, 0, slot).wait()

                @pl.when(x == 0)
                def _():
                    self.right(m, p).wait()

                self.multiply(kind, slot, p)

        for copy in self.made(i, p, x, slot):
            copy.start()

    def ready(self, w):
        self.settled(1)

        @pl.when(w == MATS - 1)
        def _():
            self.settled(0)

        s = self.s
        remote(self.pg.at[w], self.pg.at[w], s["part_send"].at[0], s["part_recv"].at[w], self.t.partner()).wait_recv()
        early, late = [], []
        for c in self.colors:
            ring = c.rings[0]
            for side in ring.sides:
                for j in range(ring.steps[side] + (side == NORTH)):
                    (late if self.consumer_lag(ring, side, j) else early).append((c, side, j))
        for c, side, j in early:
            self.start_loads(c, side, j, w)

        @pl.when(w == 0)
        def _():
            for c, side, j in late:
                self.start_loads(c, side, j, w)

    def consumer_lag(self, ring, side, j):
        c = ring.color
        if j == 0:
            e = ("s", c, 0, START, START)
        else:
            e = ("f", c, 0, side, j) if j < ring.steps[side] else ("z", c, 0, START, START)
        return self.lag[e][0]

    def start_loads(self, c, side, j, w):
        for copy in self.loads(c, side, j, w):
            copy.start()

    def sign(self, side, w):
        return (1 - 2 * lax.rem(w, 2)) * (1 - 2 * side)

    def target(self, ring, side, j, w):
        return self.t.wrap(ring.d, self.t.at[ring.d] + self.sign(side, w) * (ring.steps[side] - j))

    def loads(self, c, side, j, w):
        ring = c.rings[0]
        place = ring.message(side, j) if j < ring.steps[side] else ring.n - 1
        index = c.index(**{ring.d: self.spot(ring.d, self.target(ring, side, j, w))})
        columns = (slice(None), c.columns)
        buf, sem = self.s[f"load{c.k}"], self.s[f"load_sem{c.k}"]
        sources = self.g.at[(w, *index, *columns)], self.pg.at[(w, *index, *columns)]
        return [pltpu.make_async_copy(source, buf.at[place, n], sem.at[place, n]) for n, source in enumerate(sources)]

    def message(self, ring, side, m, w, src):
        s, name = self.s, ring.name
        n, slot = ring.message(side, m), lax.rem(w, self.slots)
        return remote(src, s["in" + name].at[slot, n], s["send" + name].at[slot, n], s["recv" + name].at[slot, n], self.t.beside(ring.d, self.sign(side, w)))

    def add(self, dst, index, ring, side, j, w, terms):
        c, s = ring.color, self.s
        if ring.phase:
            before = s["sum" + c.rings[0].name]
            own = [(before, (lax.rem(w, before.shape[0]), *c.within(self.spot(ring.d, self.target(ring, side, j, w)))))]
        else:
            place = ring.message(side, j) if j < ring.steps[side] else ring.n - 1
            for copy in self.loads(c, side, j, w):
                copy.wait()
            own = [(s[f"load{c.k}"], (place, n)) for n in range(2)]
        add_blocks(dst, index, own + terms, c.block[ring.phase])
        if not ring.phase and self.consumer_lag(ring, side, j):

            @pl.when(w + 1 < MATS)
            def _():
                self.start_loads(c, side, j, w + 1)

    def event(self, kind, c, phase, side, j, w):
        ring, s = c.rings[phase], self.s
        name, slot = ring.name, lax.rem(w, self.slots)
        box, out = s["in" + name], s["out" + name]
        part = lax.rem(w, out.shape[0])
        if kind == "s":
            for side in ring.sides:
                self.add(out, (part, side), ring, side, 0, w, [])
                self.message(ring, side, 0, w, out.at[part, side]).start()
        elif kind == "f":
            at = (slot, ring.message(side, j - 1))
            self.message(ring, side, j - 1, w, out.at[part, 0]).wait_recv()
            self.add(box, at, ring, side, j, w, [(box, at)])
            self.message(ring, side, j, w, box.at[at]).start()
        elif kind == "z":
            terms = []
            for side in ring.sides:
                m = ring.steps[side] - 1
                self.message(ring, side, m, w, out.at[part, 0]).wait_recv()
                terms.append((box, (slot, ring.message(side, m))))
            total = s["sum" + name]
            self.add(total, (lax.rem(w, total.shape[0]),), ring, NORTH, ring.steps[NORTH], w, terms)
            for side in ring.sides:
                for m in range(ring.steps[side]):
                    self.message(ring, side, m, w, out.at[part, 0]).wait_send()
        else:
            total = s["sum" + c.rings[1].name]
            last = lax.rem(w, total.shape[0])
            copies = [direct(self.t, ring, o, w, out.at[part, o - 1], box.at[slot, o - 1], s, slot, slot) for o in range(1, ring.n)]
            if kind == "d":
                for o, copy in enumerate(copies):
                    out[part, o] = total[last, self.spot(ring.d, self.t.wrap(ring.d, self.t.at[ring.d] + o + 1))].astype(bf16)
                    copy.start()
            else:
                value = total[last, self.spot(ring.d, self.t.at[ring.d])]
                for o, copy in enumerate(copies):
                    copy.wait_recv()
                    value = value + box[slot, o].astype(f32)
                self.unit[w, :, c.columns] = value
                for copy in copies:
                    copy.wait_send()

    def step(self, i, j):
        @pl.when(i < MATS)
        def _():
            self.tile(i, j)

        @pl.when((j == 0) & (i > 0) & (i <= MATS))
        def _():
            self.ready(i - 1)

        for at in range(self.tiles):

            @pl.when(j == at)
            def _():
                for e, lag, _ in sorted((n for n in self.order if n[2] == at), key=lambda n: n[1]):
                    self.turn(e, i - 1 - lag)

    def turn(self, e, w):
        @pl.when((w >= 0) & (w < MATS))
        def _():
            if e == self.first:

                @pl.when(w >= self.slots)
                def _():
                    pl.semaphore_wait(self.s["free"].at[w - self.slots], len(self.t.everyone()))

            self.event(*e, w)
            if e == self.last:

                @pl.when(w + self.slots < MATS)
                def _():
                    for device in self.t.everyone():
                        signal(self.s["free"].at[w], device)

    def run(self):
        self.left(0, 0, 0).start()
        self.right(0, 0).start()

        def body(n, _):
            self.step(lax.div(n, self.tiles), lax.rem(n, self.tiles))
            return 0

        lax.fori_loop(0, (MATS + self.slots) * self.tiles, body, 0)


CHUNK = 256
WAVES = ((1, 1), (0, 1), (0, 3), (1, 0), (0, 0), (0, 2))
SHAPES = (UNIT, DOWN)


def tiles(R, C):
    r, c = TILE
    across, wide = C // c, UNIT[1] // c
    for n in range(R * C // (r * c)):
        yield (pl.ds(n // across * r, r), pl.ds(n % across * c, c)), (pl.ds(n // wide * r, r), pl.ds(n % wide * c, c))


def exchange_scratch():
    shapes = {}
    for kind, (R, C) in enumerate(SHAPES):
        n = sum(w[0] == kind for w in WAVES)
        shapes[f"nat{kind}"] = pltpu.VMEM((R, C), f32)
        shapes[f"slab{kind}"] = pltpu.VMEM((4, n, PADS[kind], C), bf16)
        shapes[f"rows{kind}"] = pltpu.VMEM((4, n, PADS[kind], C), bf16)
    shapes["x_send"] = pltpu.SemaphoreType.DMA((2, 4))
    shapes["x_recv"] = pltpu.SemaphoreType.DMA((2, 4))
    return shapes


def exchange(t, s):
    me = lax.rem(t.idx, 4)
    copies = []
    for o in range(1, 4):
        to = lax.rem(me + o, 4)
        for kind in range(2):
            copies.append(remote(s[f"slab{kind}"].at[to], s[f"rows{kind}"].at[me], s["x_send"].at[kind, o], s["x_recv"].at[kind, o], t.group(to)))
    for copy in copies:
        copy.start()
    for kind in range(2):
        s[f"rows{kind}"][me] = s[f"slab{kind}"][me]
    for copy in copies:
        copy.wait()


def scatter_kernel(dims, names, *refs):
    take = iter(refs)
    lefts, rights, outs = ([next(take) for _ in range(n)] for n in (MATS, MATS, 2))
    g, pg = next(take), next(take)
    s = dict(zip(names, take, strict=True))
    t = Torus(dims)
    enter(t.everyone() + [t.partner(), t.crossed()])
    sc = Scatter(dims)
    sc.bind(t, lefts, rights, g, pg, s["unit"], s)
    sc.run()
    for w, (kind, at) in enumerate(WAVES):
        R, C = SHAPES[kind]
        nat, slab = s[f"nat{kind}"], s[f"slab{kind}"]
        for natural, unit in tiles(R, C):
            nat[natural] = s["unit"][(w, *unit)]
        rows = R // 4
        for q in range(4):
            slab[q, at, 0:rows, :] = nat[q * rows : (q + 1) * rows, :].astype(bf16)
    exchange(t, s)
    for kind, out in enumerate(outs):
        C = SHAPES[kind][1]
        for q in range(4):
            out[:, :, C * q : C * (q + 1)] = s[f"rows{kind}"][q]


def places():
    return pl.BlockSpec(memory_space=pl.ANY), pl.BlockSpec(memory_space=pltpu.VMEM)


def scatter(factors, dims):
    sc = Scatter(dims)
    sc.tokens = factors[0][0].shape[0]
    scratch = sc.scratch() | {"unit": pltpu.VMEM((MATS, *UNIT), f32)} | exchange_scratch()
    anywhere, vmem = places()
    rows = [jax.ShapeDtypeStruct((sum(w[0] == kind for w in WAVES), PADS[kind], 4 * C), bf16) for kind, (_, C) in enumerate(SHAPES)]
    terms = jax.ShapeDtypeStruct((MATS, *dims, *UNIT), bf16)
    *grads, _, _ = pl.pallas_call(
        functools.partial(scatter_kernel, dims, tuple(scratch)),
        out_shape=(*rows, terms, terms),
        in_specs=[anywhere] * 2 * MATS,
        out_specs=(vmem, vmem, anywhere, anywhere),
        scratch_shapes=list(scratch.values()),
        compiler_params=pltpu.CompilerParams(collective_id=1, has_side_effects=True, vmem_limit_bytes=VMEM_MOST),
        name="scatter",
    )(*[left for left, _ in factors], *[right for _, right in factors])
    return grads


class Gather:
    def __init__(self, dims):
        self.colors = [Color(k, dims) for k in range(len(ORDERS))]
        events = [e for c in self.colors for e in c.events(True)]
        timed = []
        for n, (e, character) in enumerate(zip(events, GATHER_TIMES, strict=True)):
            for w in range(MATS):
                timed.append((time_of(character) + GATHER_STEPS[e[2] == START] * w, w, n))
        self.order = [(events[n], w) for _, w, n in sorted(timed)]

    def scratch(self):
        shapes = {}
        for c in self.colors:
            for ring in c.rings:
                for way in ("send", "recv"):
                    shapes[way + ring.name] = pltpu.SemaphoreType.DMA((MATS, ring.n - 1))
        for name in ("over_send", "over_recv"):
            shapes[name] = pltpu.SemaphoreType.DMA((MATS, len(ORDERS)))
        shapes["own"] = pltpu.SemaphoreType.DMA((MATS,))
        return shapes

    def bind(self, torus, out, unit, s):
        self.t, self.out, self.unit, self.s = torus, out, unit, s

    def place(self, c, w, core, **at):
        return self.out[w].at[(*c.index(**at), core, slice(None), c.columns)]

    def own(self, w):
        t = self.t
        return pltpu.make_async_copy(self.unit.at[w], self.out[w].at[(*t.at.values(), t.core)], self.s["own"].at[w])

    def directs(self, ring, w):
        c, t = ring.color, self.t
        src, dst = self.unit.at[w, :, c.columns], self.place(c, w, t.core, **t.at)
        return [direct(t, ring, o, w, src, dst, self.s, w, w) for o in range(1, ring.n)]

    def message(self, ring, side, m, w):
        t, c, s = self.t, ring.color, self.s
        sign = (1 - 2 * side) * (1 - 2 * (w % 2))
        at = {d: t.at[d] for d in c.order[: ring.phase]} | {ring.d: t.wrap(ring.d, t.at[ring.d] - sign * m)}
        block, n = self.place(c, w, t.core, **at), ring.message(side, m)
        return remote(block, block, s["send" + ring.name].at[w, n], s["recv" + ring.name].at[w, n], t.beside(ring.d, sign))

    def over(self, c, w, core, **at):
        block = self.place(c, w, core, **at)
        return remote(block, block, self.s["over_send"].at[w, c.k], self.s["over_recv"].at[w, c.k], self.t.partner())

    def event(self, kind, c, phase, side, j, w):
        ring, t = c.rings[phase], self.t
        if kind == "d":
            for copy in self.directs(ring, w):
                copy.start()
        elif kind == "e":
            for copy in self.directs(ring, w):
                copy.wait_recv()
        elif kind == "s":
            for side in ring.sides:
                self.message(ring, side, 0, w).start()
            if not phase:
                self.over(c, w, t.core, **{ring.d: t.at[ring.d]}).start()
        else:
            self.message(ring, side, j - 1, w).wait_recv()
            if j < ring.steps[side]:
                self.message(ring, side, j, w).start()
            if not phase:
                sign = (1 - 2 * side) * (1 - 2 * (w % 2))
                self.over(c, w, t.core, **{ring.d: t.wrap(ring.d, t.at[ring.d] - sign * j)}).start()

    def finish(self, w):
        for c in self.colors:
            for ring in c.rings:
                if ring.phase == 2:
                    for copy in self.directs(ring, w):
                        copy.wait_send()
                else:
                    for side in ring.sides:
                        for m in range(ring.steps[side]):
                            self.message(ring, side, m, w).wait_send()
            self.over(c, w, self.t.core).wait_send()
            self.over(c, w, 1 - self.t.core).wait_recv()

    def run(self):
        for w in range(MATS):
            self.own(w).wait()
        for e, w in self.order:
            self.event(*e, w)
        for w in range(MATS):
            self.finish(w)


class Exchange:
    def __init__(self, t, dims):
        X, Y, Z = dims
        near = t.cores * Z
        self.t, self.steps = t, ((near, 1, near), (X * Y, near, X * Y))

    def beside(self, n, offset):
        size, stride, _ = self.steps[n]
        idx = self.t.idx
        at = lax.rem(lax.div(idx, stride), size)
        return (self.t.rep, idx + (lax.rem(at + offset, size) - at) * stride)

    def devices(self):
        return [self.beside(n, o) for n, (size, *_) in enumerate(self.steps) for o in range(1, size)]

    def total(self, s, value):
        for n, (size, *_) in enumerate(self.steps):
            mine, box = s["norm_out"].at[n], s["norm_in"].at[n]
            mine[...] = value
            copies = [remote(mine, box.at[o], s["norm_send"].at[n, o], s["norm_recv"].at[n, o], self.beside(n, o)) for o in range(1, size)]
            for copy in copies:
                copy.start()
            for copy in copies:
                copy.wait()
            value = value + sum(box[o] for o in range(1, size))
        return value


def moments_of(g, m, v):
    return 0.9 * m + 0.1 * g, 0.95 * v + 0.05 * g * g


def rows_of(grads, kind, at):
    which, layer = (2, at) if kind else divmod(at, 2)
    return grads[kind][at, 0 : SHAPES[kind][0] // 4, :].astype(f32), which, layer


def update_kernel(dims, names, *refs):
    take = iter(refs)
    grads, w_in, m_in, v_in = ([next(take) for _ in range(n)] for n in (2, 3, 3, 3))
    factor_out, out = next(take), [next(take) for _ in WAVES]
    s = dict(zip(names, take, strict=True))
    t = Torus(dims)
    ex = Exchange(t, dims)
    enter(ex.devices())
    total, count = jnp.zeros((1, 1), f32), 0
    for kind, at in WAVES:
        g, *_ = rows_of(grads, kind, at)
        total = total + jnp.sum(jnp.sum(g * g, axis=0, keepdims=True), axis=1, keepdims=True)
        count += g.size
    for size, *_ in ex.steps:
        count *= size
    total = ex.total(s, jnp.broadcast_to(total, TILE))
    factor_out[...] = jnp.minimum(1.0, 0.5 * lax.rsqrt(total / count + 1e-30))
    factor = factor_out[0:1, 0:1]
    for kind, at in WAVES:
        g, which, layer = rows_of(grads, kind, at)
        R, C = SHAPES[kind]
        w = w_in[which][layer].astype(f32)
        m, v = moments_of(g * factor, m_in[which][:, layer, :], v_in[which][:, layer, :])
        w = (w - 0.02 * (m * lax.rsqrt(v + 1e-8) + 0.1 * w)).astype(bf16)
        for q in range(4):
            s[f"slab{kind}"][q, at, 0 : R // 4, :] = w[:, C * q : C * (q + 1)]
    exchange(t, s)
    ga = Gather(dims)
    ga.bind(t, out, s["unit"], s)
    for w, (kind, at) in enumerate(WAVES):
        R, C = SHAPES[kind]
        nat, rows_in, n = s[f"nat{kind}"], s[f"rows{kind}"], R // 4
        for q in range(4):
            nat[q * n : (q + 1) * n, :] = rows_in[q, at, 0:n, :].astype(f32)
        for natural, unit in tiles(R, C):
            s["wide"][unit] = nat[natural]
        s["unit"][w] = s["wide"][...].astype(bf16)
        ga.own(w).start()
    ga.run()


IN_VMEM = (0, 1, 2, 3)


def home(wave):
    return pltpu.VMEM if wave in IN_VMEM else pltpu.HBM


def update(grads, w, moments, dims):
    X, Y, Z = dims
    scratch = Gather(dims).scratch() | exchange_scratch()
    scratch["unit"] = pltpu.VMEM((MATS, *UNIT), bf16)
    scratch["wide"] = pltpu.VMEM(UNIT, f32)
    most = max(2 * Z, X * Y)
    scratch["norm_out"] = pltpu.VMEM((2, *TILE), f32)
    scratch["norm_in"] = pltpu.VMEM((2, most, *TILE), f32)
    for name in ("norm_send", "norm_recv"):
        scratch[name] = pltpu.SemaphoreType.DMA((2, most))
    anywhere, vmem = places()
    given = (*grads, *w, *moments)
    factor, *out = pl.pallas_call(
        functools.partial(update_kernel, dims, tuple(scratch)),
        out_shape=[jax.ShapeDtypeStruct(TILE, f32)] + [home(wave)((*dims, 2, *UNIT), bf16) for wave in range(MATS)],
        in_specs=[vmem] * len(given),
        out_specs=[vmem] + [anywhere] * MATS,
        scratch_shapes=list(scratch.values()),
        compiler_params=pltpu.CompilerParams(collective_id=2, has_side_effects=True, vmem_limit_bytes=VMEM_FEW),
        name="update",
    )(*given)
    return factor, out


VMEM_MOST, VMEM_FEW = 62 << 20, 12 << 20


def normed(h):
    wide = h.astype(f32)
    scale = lax.rsqrt(jnp.mean(wide**2, -1, keepdims=True) + 1e-6)
    return (wide * scale).astype(bf16)


def norm_back(h, da):
    wide, da = h.astype(f32), da.astype(f32)
    scale = lax.rsqrt(jnp.mean(wide**2, -1, keepdims=True) + 1e-6)
    inner = jnp.mean(wide * da, -1, keepdims=True)
    return (scale * da - wide * (inner * scale * scale * scale)).astype(bf16)


PLAIN, TURNED = ((1,), (0,)), ((1,), (1,))
ROWS = 128


def dot(a, b, dims):
    return lax.dot_general(a, b, (dims, ((), ())), preferred_element_type=f32)


def by_rows(ref, work):
    def some(i, _):
        work(pl.ds(pl.multiple_of(i * ROWS, ROWS), ROWS))
        return 0

    lax.fori_loop(0, ref.shape[0] // ROWS, some, 0)


def gate_back(dhid, gate, up):
    soft = jax.nn.sigmoid(gate)
    return dhid * up * (soft * (1.0 + gate * (1.0 - soft))), dhid * (gate * soft)


def bottom_kernel(h, wg, wu, wd, a, gate, up, hid, out, acc):
    step = pl.program_id(0)

    @pl.when(step == 0)
    def _():
        def first(rows):
            a[rows] = normed(h[rows])
            acc[rows] = jnp.zeros_like(acc[rows])

        by_rows(h, first)

    for part in parts():
        gate[:, part] = dot(a[...], wg[0, :, part], PLAIN)
        up[:, part] = dot(a[...], wu[0, :, part], PLAIN)
        hid[:, part] = (jax.nn.silu(gate[:, part]) * up[:, part]).astype(bf16)
    acc[...] += dot(hid[...], wd[0], PLAIN)

    @pl.when(step == pl.num_programs(0) - 1)
    def _():
        def last(rows):
            out[rows] = h[rows] + acc[rows].astype(bf16)

        by_rows(h, last)


def top_kernel(h, dy, wg, wu, wd, a, hid, dgate, dup, dh, acc_gate, acc_up):
    step = pl.program_id(0)

    @pl.when(step == 0)
    def _():
        def first(rows):
            a[rows] = normed(h[rows])
            for acc in (acc_gate, acc_up):
                acc[rows] = jnp.zeros_like(acc[rows])

        by_rows(h, first)

    for part in parts():
        gate = dot(a[...], wg[0, :, part], PLAIN)
        up = dot(a[...], wu[0, :, part], PLAIN)
        dhid = dot(dy[...], wd[0, part, :], TURNED).astype(bf16).astype(f32)
        hid[:, part] = (jax.nn.silu(gate) * up).astype(bf16)
        by_gate, by_up = gate_back(dhid, gate, up)
        dgate[:, part], dup[:, part] = by_gate.astype(bf16), by_up.astype(bf16)
    for acc, d, w in ((acc_gate, dgate, wg), (acc_up, dup, wu)):
        acc[...] += dot(d[...], w[0], TURNED)

    @pl.when(step == pl.num_programs(0) - 1)
    def _():
        def last(rows):
            da = acc_gate[rows].astype(bf16) + acc_up[rows].astype(bf16)
            dh[rows] = dy[rows] + norm_back(h[rows], da)

        by_rows(h, last)


def back_kernel(dh, gate, up, wd, dgate, dup):
    for part in parts():
        dhid = dot(dh[...], wd[0, part, :], TURNED).astype(bf16).astype(f32)
        by_gate, by_up = gate_back(dhid, gate[:, part], up[:, part])
        dgate[:, part], dup[:, part] = by_gate.astype(bf16), by_up.astype(bf16)


WIDTH, PART = 512, 256


def parts():
    return [slice(at, at + PART) for at in range(0, WIDTH, PART)]


def layer_call(kernel, layer, tokens_in, hidden_in, weights, hidden_out, tokens_out, accumulators, products, name):
    T, D = tokens_in[0].shape
    FF = weights[-1].shape[1]
    whole = pl.BlockSpec((T, D), lambda n: (0, 0))
    part = pl.BlockSpec((T, WIDTH), lambda n: (0, n))
    specs = [pl.BlockSpec((1, D, WIDTH), lambda n: (layer, 0, n))] * (len(weights) - 1) + [pl.BlockSpec((1, WIDTH, D), lambda n: (layer, n, 0))]
    early, late = tokens_out
    shape = jax.ShapeDtypeStruct
    return pl.pallas_call(
        kernel,
        grid=(FF // WIDTH,),
        in_specs=[whole] * len(tokens_in) + [part] * len(hidden_in) + specs,
        out_specs=[whole] * early + [part] * len(hidden_out) + [whole] * late,
        out_shape=[shape((T, D), bf16)] * early + [shape((T, FF), t) for t in hidden_out] + [shape((T, D), bf16)] * late,
        scratch_shapes=[pltpu.VMEM((T, D), f32)] * accumulators,
        cost_estimate=pl.CostEstimate(flops=2 * products * T * D * FF, bytes_accessed=2 * len(weights) * D * FF, transcendentals=T * FF),
        compiler_params=pltpu.CompilerParams(vmem_limit_bytes=VMEM_MOST),
        name=name,
    )(*tokens_in, *hidden_in, *weights)


def factors(x, dy, wg, wu, wd):
    weights = (wg, wu, wd)
    a0, gate, up, hid0, h = layer_call(bottom_kernel, 0, (x,), (), weights, (f32, f32, bf16), (1, 1), 1, 3, "bottom")
    a1, hid1, dg1, du1, dh = layer_call(top_kernel, 1, (h, dy), (), weights, (bf16,) * 3, (1, 1), 2, 5, "top")
    dg0, du0 = layer_call(back_kernel, 0, (dh,), (gate, up), (wd,), (bf16,) * 2, (0, 0), 0, 1, "back")
    return (hid1, dy), (a1, dg1), (a1, du1), (hid0, dh), (a0, dg0), (a0, du0)


SETTLED = (4, 1, 5, 2, 3, 0)
BOXES = 3


def pieces(kind):
    runs = []
    for (rows, columns), (unit_rows, unit_columns) in tiles(*SHAPES[kind]):
        if runs and runs[-1][:2] == [rows, unit_rows]:
            runs[-1][-1] += columns.size
        else:
            runs.append([rows, unit_rows, columns.start, unit_columns.start, columns.size])
    return runs


def settle_kernel(*refs):
    take = iter(refs)
    waves, grads, m_in, v_in, outs, m_out, v_out = ([next(take) for _ in range(n)] for n in (MATS, 2, 3, 3, 3, 3, 3))
    factor, box, in_sem, out_sem, near_sem = next(take), *take
    X = waves[0].shape[0]

    def put(n, x, q, block, sem):
        kind = WAVES[SETTLED[n]][0]
        C = SHAPES[kind][1]
        for rows, unit_rows, column, unit_column, width in pieces(kind):
            to = outs[n // 2].at[n % 2, x, :, :, rows, pl.ds(pl.multiple_of(C * q + column, TILE[1]), width)]
            pltpu.make_async_copy(block.at[:, :, lax.div(q, 2), lax.rem(q, 2), unit_rows, pl.ds(unit_column, width)], to, sem).start()

    def all_of(n, x, block, sem):
        lax.fori_loop(0, 4, lambda q, _: (put(n, x, q, block, sem), 0)[1], 0)

    near = [n for n, w in enumerate(SETTLED) if w in IN_VMEM]
    far = [(n, x) for n in range(MATS) if n not in near for x in range(X)]

    def fetch(k):
        n, x = far[k]
        return pltpu.make_async_copy(waves[n].at[x], box.at[k % BOXES], in_sem.at[k % BOXES])

    def drain(k):
        n, x = far[k]
        pltpu.make_async_copy(box.at[k % BOXES], waves[n].at[x], out_sem.at[k % BOXES]).wait()

    ahead = BOXES - 1
    for k in range(ahead):
        fetch(k).start()
    for n in near:
        lax.fori_loop(0, X, lambda x, _: (all_of(n, x, waves[n].at[x], near_sem.at[n]), 0)[1], 0)
    for kind, at in WAVES:
        g, which, layer = rows_of(grads, kind, at)
        m, v = moments_of(g * factor[0:1, 0:1], m_in[which][:, layer, :], v_in[which][:, layer, :])
        m_out[which][:, layer, :], v_out[which][:, layer, :] = m, v
    for k in range(len(far)):
        fetch(k).wait()
        all_of(*far[k], box.at[k % BOXES], out_sem.at[k % BOXES])
        if k + ahead < len(far):
            if k:
                drain(k - 1)
            fetch(k + ahead).start()
    for k in range(len(far) - BOXES, len(far)):
        drain(k)
    for n in near:
        pltpu.make_async_copy(waves[n], waves[n], near_sem.at[n]).wait()


def settle(waves, factor, grads, moments, dims):
    X, Y, Z = dims
    halves = Z // 2
    shape = (X, Y, halves, 2, 2, *UNIT)
    anywhere, vmem = places()
    made = jax.ShapeDtypeStruct
    R, C = zip(*SHAPES)
    outs = pl.pallas_call(
        lambda *refs: settle_kernel(*refs[: MATS + 2 + len(moments)], *refs[MATS + 3 + len(moments) : -4], refs[MATS + 2 + len(moments)], *refs[-4:]),
        out_shape=[made((2, X, Y, halves, R[which // 2], 4 * C[which // 2]), bf16) for which in range(3)] + [made(a.shape, f32) for a in moments],
        in_specs=[vmem if n in IN_VMEM else anywhere for n in SETTLED] + [vmem] * (3 + len(moments)),
        out_specs=[anywhere] * 3 + [vmem] * len(moments),
        scratch_shapes=[pltpu.VMEM((BOXES, *shape[1:]), bf16)] + [pltpu.SemaphoreType.DMA((n,)) for n in (BOXES, BOXES, MATS)],
        compiler_params=pltpu.CompilerParams(vmem_limit_bytes=VMEM_FEW),
        name="settle",
    )(*[pltpu.with_memory_space_constraint(waves[n].reshape(shape), home(n)) for n in SETTLED], *grads, *moments, factor)
    return [out.reshape(2, -1, out.shape[-1]) for out in outs[:3]], outs[3:]


def device_step(dims, x, dy, wg, wu, wd, *moments):
    grads = scatter(factors(x[0], dy[0], wg, wu, wd), dims)
    place = lax.axis_index("dp")
    w = [lax.dynamic_slice_in_dim(a, place * b.shape[1], b.shape[1], 1) for a, b in zip((wg, wu, wd), moments[:3], strict=True)]
    moments = [jnp.swapaxes(a, 0, 1) for a in moments]
    factor, waves = update(grads, w, moments, dims)
    new, moments = settle(waves, factor, grads, moments, dims)
    return (*new, *[jnp.swapaxes(a, 0, 1) for a in moments])


DIMS = {256: (4, 4, 8)}


def solution(mesh):
    dims = DIMS[mesh.shape["dp"]]
    spec = jax.sharding.PartitionSpec
    tokens, whole, rows = spec(("rep", "dp")), spec(), spec(None, "dp", None)
    return jax.shard_map(
        functools.partial(device_step, dims),
        mesh=mesh,
        in_specs=(tokens, tokens, *[whole] * 3, *[rows] * 6),
        out_specs=(*[spec("rep")] * 3, *[spec("rep", "dp", None)] * 6),
        check_vma=False,
    )
```

```python
import functools
import jax, jax.numpy as jnp
from jax import lax
from jax.experimental import pallas as pl
from jax.experimental.pallas import tpu as pltpu

bf16, f32 = jnp.bfloat16, jnp.float32
MATS = 6
UNIT = (24, 896)
DOWN = (56, 384)
TILE = (8, 128)
PADS = (8, 16)
ORDERS = ("xyz", "yzx", "zxy")
COLUMNS = ((0, 384), (384, 256), (640, 256))
KINDS = ("s", "f", "z", "d", "e")
SCATTER_TIMES = '$*115::B$)-/12479;;A$()+-0339<<A'
GATHER_TIMES, GATHER_STEPS = '$119???`j~$44>>EEQRYYeoo#))2IIISZ`ijxx', (4, 14)
MESH = pl.DeviceIdType.MESH
START, MORE = 0, 1
NORTH, SOUTH = 0, 1


def time_of(character):
    return ord(character) - ord("#")


class Torus:
    def __init__(self, dims):
        self.dims = dict(zip("xyz", dims))
        self.cores = 2
        _, Y, Z = dims
        self.stride = dict(zip("xyz", (Y * Z * self.cores, Z * self.cores, self.cores)))
        self.rep, self.idx = lax.axis_index("rep"), lax.axis_index("dp")
        self.at = {d: lax.rem(lax.div(self.idx, self.stride[d]), self.dims[d]) for d in "xyz"}
        self.core = lax.rem(self.idx, self.cores)

    def wrap(self, d, value):
        n = self.dims[d]
        return lax.rem(value + n, n)

    def beside(self, d, offset):
        return (self.rep, self.idx + (self.wrap(d, self.at[d] + offset) - self.at[d]) * self.stride[d])

    def partner(self):
        return (self.rep, self.idx + 1 - 2 * self.core)

    def everyone(self):
        return [self.beside(d, o) for d in "xyz" for o in range(1, self.dims[d])]

    def group(self, s):
        return (self.rep, self.idx - lax.rem(self.idx, 4) + s)

    def crossed(self):
        return self.group(lax.rem(lax.rem(self.idx, 4) + 3 - 2 * self.core, 4))


def enter(devices):
    barrier = pltpu.get_barrier_semaphore()
    for device in devices:
        signal(barrier, device)
    pl.semaphore_wait(barrier, len(devices))


def signal(sem, device):
    pl.semaphore_signal(sem, inc=1, device_id=device, device_id_type=MESH)


def remote(src, dst, send, recv, device):
    return pltpu.make_async_remote_copy(src_ref=src, dst_ref=dst, send_sem=send, recv_sem=recv, device_id=device, device_id_type=MESH)


class Ring:
    def __init__(self, color, phase, d, n):
        self.name = f"{color.k}{phase}"
        self.color, self.phase, self.d, self.n = color, phase, d, n
        self.steps = (n // 2, (n - 1) // 2)
        self.sides = [side for side in (NORTH, SOUTH) if self.steps[side]]

    def message(self, side, m):
        return m + side * self.steps[NORTH]


class Color:
    def __init__(self, k, dims):
        self.k, self.order = k, ORDERS[k]
        start, self.width = COLUMNS[k]
        self.columns = pl.ds(start, self.width)
        size = dict(zip("xyz", dims))
        n = [size[d] for d in self.order]
        self.rings = [Ring(self, phase, d, m) for phase, (d, m) in enumerate(zip(self.order, n))]
        first, second, third = self.order
        self.rest = [d for d in "xyz" if d != first]
        self.block = (tuple(size[d] for d in self.rest), (size[third],))
        self.unit = (UNIT[0], self.width)

    def index(self, **at):
        return tuple(at.get(d, slice(None)) for d in "xyz")

    def within(self, b):
        return tuple(b if d == self.order[1] else slice(None) for d in self.rest)

    def events(self, gather):
        rings, direct = [], [("d", self, 2, START, START), ("e", self, 2, START, START)]
        for ring in self.rings[:2][:: -1 if gather else 1]:
            rings.append(("s", self, ring.phase, START, START))
            for j in range(1, ring.steps[NORTH] + gather):
                rings += [("f", self, ring.phase, side, j) for side in (NORTH, SOUTH) if side == NORTH or j < ring.steps[SOUTH] + gather]
            if not gather:
                rings.append(("z", self, ring.phase, START, START))
        return direct + rings if gather else rings + direct


def add_blocks(dst, dst_index, terms, shape):
    def at(ref, index, place):
        place = list(place)
        return ref[tuple([place.pop(0) if isinstance(e, slice) else e for e in index] + place)]

    def row(i, _):
        for rest in [(j,) for n in shape[1:] for j in range(n)] or [()]:
            place = (i, *rest)
            dst[(*dst_index, *place)] = sum(at(ref, index, place).astype(f32) for ref, index in terms).astype(dst.dtype)
        return 0

    lax.fori_loop(0, shape[0], row, 0)


def direct(t, ring, o, w, src, dst, s, slot, half):
    name = ring.name
    return remote(src, dst, s["send" + name].at[half, o - 1], s["recv" + name].at[slot, o - 1], t.beside(ring.d, o))


class Scatter:
    def __init__(self, dims):
        self.dims = dims
        self.X, self.Y, Z = dims
        self.halves = Z // 2
        self.tiles = 2 * self.X
        self.colors = [Color(k, dims) for k in range(len(ORDERS))]
        events = [e for c in self.colors for e in c.events(False)]
        lag = [divmod(time_of(c), self.tiles) for c in SCATTER_TIMES]
        self.order = [(e, *when) for e, when in zip(events, lag, strict=True)]
        self.lag = {e: when for e, *when in self.order}
        self.depth = max(lag for _, lag, _ in self.order)
        self.slots = self.depth + 1
        self.first = min((e for e in events if e[0] == "s" and not e[2]), key=lambda e: (*self.lag[e], events.index(e)))
        self.last = max((e for e in events if e[0] == "e"), key=lambda e: (*self.lag[e], events.index(e)))

    def scratch(self):
        shapes = {}
        NS = self.slots
        for c in self.colors:
            for ring in c.rings:
                n, name = ring.n, ring.name
                block = (c.block + ((),))[ring.phase] + c.unit
                shapes["recv" + name] = pltpu.SemaphoreType.DMA((NS, n - 1))
                shapes["send" + name] = pltpu.SemaphoreType.DMA((NS, n - 1))
                shapes["in" + name] = pltpu.VMEM((NS, n - 1) + block, bf16)
                shapes["out" + name] = pltpu.VMEM((self.kept(c, ring.phase, "s" if ring.phase < 2 else "d"), len(ring.sides) if ring.phase < 2 else n - 1) + block, bf16)
                if ring.phase < 2:
                    shapes["sum" + name] = pltpu.VMEM((self.kept(c, ring.phase, "z"),) + block, f32)
            n = c.rings[0].n
            shapes[f"load{c.k}"] = pltpu.VMEM((n, 2) + c.block[0] + c.unit, bf16)
            shapes[f"load_sem{c.k}"] = pltpu.SemaphoreType.DMA((n, 2))
        for name in ("part_send", "own", "left_sem", "right_sem"):
            shapes[name] = pltpu.SemaphoreType.DMA((2,))
        shapes["part_recv"] = pltpu.SemaphoreType.DMA((MATS,))
        shapes["left"] = pltpu.VMEM((2, self.tokens, self.Y * self.halves * DOWN[0]), bf16)
        shapes["right"] = pltpu.VMEM((2, self.tokens, 2 * UNIT[1]), bf16)
        shapes["stage"] = pltpu.VMEM((2, self.Y, self.halves, 2, *UNIT), bf16)
        shapes["free"] = pltpu.SemaphoreType.REGULAR((MATS,))
        return shapes

    def lags(self, c, phase, kinds):
        return [lag for e, lag, _ in self.order if e[1] is c and e[2] == phase and e[0] in kinds]

    def kept(self, c, phase, kind):
        if kind == "s":
            ends = self.lags(c, phase, "z")
        elif kind == "d":
            ends = self.lags(c, phase, "e")
        else:
            ends = self.lags(c, phase + 1, "ze")
        return max(ends) - min(self.lags(c, phase, kind)) + 1

    def bind(self, torus, lefts, rights, g, pg, unit, s):
        self.t, self.lefts, self.rights, self.g, self.pg, self.unit, self.s = torus, lefts, rights, g, pg, unit, s

    def spot(self, d, place):
        return lax.rem(place, 2) * self.halves + lax.div(place, 2) if d == "z" else place


    def left(self, m, x, slot):
        width = self.Y * self.halves * SHAPES[WAVES[m][0]][0]
        source = self.lefts[m].at[:, pl.ds(pl.multiple_of(x * width, width), width)]
        return pltpu.make_async_copy(source, self.s["left"].at[slot, :, pl.ds(0, width)], self.s["left_sem"].at[slot])

    def right(self, m, p):
        width = 2 * SHAPES[WAVES[m][0]][1]
        source = self.rights[m].at[:, pl.ds(p * width, width)]
        return pltpu.make_async_copy(source, self.s["right"].at[p, :, pl.ds(0, width)], self.s["right_sem"].at[p])

    def made(self, m, p, x, slot):
        t, s, stage = self.t, self.s, self.s["stage"]
        place = (m, x, slice(None), pl.ds(p * self.halves, self.halves))
        own = pltpu.make_async_copy(stage.at[slot, :, :, t.core], self.g.at[place], s["own"].at[slot])
        return own, remote(stage.at[slot, :, :, 1 - t.core], self.pg.at[place], s["part_send"].at[slot], s["part_recv"].at[m], t.partner())

    def settled(self, slot):
        own, theirs = self.made(0, 0, 0, slot)
        own.wait()
        theirs.wait_send()

    def multiply(self, kind, slot, p):
        R, C = SHAPES[kind]
        left, right, out = self.s["left"], self.s["right"], self.s["stage"]
        for start in range(0, 2 * C, CHUNK):
            wide = lax.dot_general(left[slot, :, 0 : self.Y * self.halves * R], right[p, :, start : start + CHUNK], (((0,), (0,)), ((), ())), preferred_element_type=f32)
            wide = wide.reshape(self.Y, self.halves, R, CHUNK)
            for core in range(2):
                if kind:
                    for natural, unit in tiles(*DOWN):
                        at = core * C + natural[1].start - start
                        if 0 <= at < CHUNK:
                            rows = slice(natural[0].start, natural[0].start + natural[0].size)
                            out[(slot, slice(None), slice(None), core, *unit)] = wide[:, :, rows, at : at + natural[1].size].astype(bf16)
                else:
                    begin, end = max(start, core * C), min(start + CHUNK, core * C + C)
                    if begin < end:
                        out[slot, :, :, core, :, begin - core * C : end - core * C] = wide[..., begin - start : end - start].astype(bf16)

    def tile(self, i, j):
        X = self.X
        slot, p, x = lax.rem(j, 2), lax.div(j, X), lax.rem(j, X)
        then = j + 1 == self.tiles
        following, beside = i + then.astype(jnp.int32), jnp.where(then, 0, j + 1)
        for m in range(MATS):

            @pl.when(following == m)
            def _():
                self.left(m, lax.rem(beside, X), lax.rem(beside, 2)).start()

            @pl.when((j == 0) & (i == m))
            def _():
                self.right(m, 1).start()

            @pl.when((j == X) & (i + 1 == m))
            def _():
                self.right(m, 0).start()

        @pl.when((j != 1) & (i + j > 0))
        def _():
            self.settled(slot)

        for m, kind in enumerate(k for k, _ in WAVES[:2]):

            @pl.when((lax.rem(i, 3) == 0) == (m == 0))
            def _():
                self.left(m, 0, slot).wait()

                @pl.when(x == 0)
                def _():
                    self.right(m, p).wait()

                self.multiply(kind, slot, p)

        for copy in self.made(i, p, x, slot):
            copy.start()

    def ready(self, w):
        self.settled(1)

        @pl.when(w == MATS - 1)
        def _():
            self.settled(0)

        s = self.s
        remote(self.pg.at[w], self.pg.at[w], s["part_send"].at[0], s["part_recv"].at[w], self.t.partner()).wait_recv()
        early, late = [], []
        for c in self.colors:
            ring = c.rings[0]
            for side in ring.sides:
                for j in range(ring.steps[side] + (side == NORTH)):
                    (late if self.consumer_lag(ring, side, j) else early).append((c, side, j))
        for c, side, j in early:
            self.start_loads(c, side, j, w)

        @pl.when(w == 0)
        def _():
            for c, side, j in late:
                self.start_loads(c, side, j, w)

    def consumer_lag(self, ring, side, j):
        c = ring.color
        if j == 0:
            e = ("s", c, 0, START, START)
        else:
            e = ("f", c, 0, side, j) if j < ring.steps[side] else ("z", c, 0, START, START)
        return self.lag[e][0]

    def start_loads(self, c, side, j, w):
        for copy in self.loads(c, side, j, w):
            copy.start()

    def sign(self, side, w):
        return (1 - 2 * lax.rem(w, 2)) * (1 - 2 * side)

    def target(self, ring, side, j, w):
        return self.t.wrap(ring.d, self.t.at[ring.d] + self.sign(side, w) * (ring.steps[side] - j))

    def loads(self, c, side, j, w):
        ring = c.rings[0]
        place = ring.message(side, j) if j < ring.steps[side] else ring.n - 1
        index = c.index(**{ring.d: self.spot(ring.d, self.target(ring, side, j, w))})
        columns = (slice(None), c.columns)
        buf, sem = self.s[f"load{c.k}"], self.s[f"load_sem{c.k}"]
        sources = self.g.at[(w, *index, *columns)], self.pg.at[(w, *index, *columns)]
        return [pltpu.make_async_copy(source, buf.at[place, n], sem.at[place, n]) for n, source in enumerate(sources)]

    def message(self, ring, side, m, w, src):
        s, name = self.s, ring.name
        n, slot = ring.message(side, m), lax.rem(w, self.slots)
        return remote(src, s["in" + name].at[slot, n], s["send" + name].at[slot, n], s["recv" + name].at[slot, n], self.t.beside(ring.d, self.sign(side, w)))

    def add(self, dst, index, ring, side, j, w, terms):
        c, s = ring.color, self.s
        if ring.phase:
            before = s["sum" + c.rings[0].name]
            own = [(before, (lax.rem(w, before.shape[0]), *c.within(self.spot(ring.d, self.target(ring, side, j, w)))))]
        else:
            place = ring.message(side, j) if j < ring.steps[side] else ring.n - 1
            for copy in self.loads(c, side, j, w):
                copy.wait()
            own = [(s[f"load{c.k}"], (place, n)) for n in range(2)]
        add_blocks(dst, index, own + terms, c.block[ring.phase])
        if not ring.phase and self.consumer_lag(ring, side, j):

            @pl.when(w + 1 < MATS)
            def _():
                self.start_loads(c, side, j, w + 1)

    def event(self, kind, c, phase, side, j, w):
        ring, s = c.rings[phase], self.s
        name, slot = ring.name, lax.rem(w, self.slots)
        box, out = s["in" + name], s["out" + name]
        part = lax.rem(w, out.shape[0])
        if kind == "s":
            for side in ring.sides:
                self.add(out, (part, side), ring, side, 0, w, [])
                self.message(ring, side, 0, w, out.at[part, side]).start()
        elif kind == "f":
            at = (slot, ring.message(side, j - 1))
            self.message(ring, side, j - 1, w, out.at[part, 0]).wait_recv()
            self.add(box, at, ring, side, j, w, [(box, at)])
            self.message(ring, side, j, w, box.at[at]).start()
        elif kind == "z":
            terms = []
            for side in ring.sides:
                m = ring.steps[side] - 1
                self.message(ring, side, m, w, out.at[part, 0]).wait_recv()
                terms.append((box, (slot, ring.message(side, m))))
            total = s["sum" + name]
            self.add(total, (lax.rem(w, total.shape[0]),), ring, NORTH, ring.steps[NORTH], w, terms)
            for side in ring.sides:
                for m in range(ring.steps[side]):
                    self.message(ring, side, m, w, out.at[part, 0]).wait_send()
        else:
            total = s["sum" + c.rings[1].name]
            last = lax.rem(w, total.shape[0])
            copies = [direct(self.t, ring, o, w, out.at[part, o - 1], box.at[slot, o - 1], s, slot, slot) for o in range(1, ring.n)]
            if kind == "d":
                for o, copy in enumerate(copies):
                    out[part, o] = total[last, self.spot(ring.d, self.t.wrap(ring.d, self.t.at[ring.d] + o + 1))].astype(bf16)
                    copy.start()
            else:
                value = total[last, self.spot(ring.d, self.t.at[ring.d])]
                for o, copy in enumerate(copies):
                    copy.wait_recv()
                    value = value + box[slot, o].astype(f32)
                self.unit[w, :, c.columns] = value
                for copy in copies:
                    copy.wait_send()

    def step(self, i, j):
        @pl.when(i < MATS)
        def _():
            self.tile(i, j)

        @pl.when((j == 0) & (i > 0) & (i <= MATS))
        def _():
            self.ready(i - 1)

        for at in range(self.tiles):

            @pl.when(j == at)
            def _():
                for e, lag, _ in sorted((n for n in self.order if n[2] == at), key=lambda n: n[1]):
                    self.turn(e, i - 1 - lag)

    def turn(self, e, w):
        @pl.when((w >= 0) & (w < MATS))
        def _():
            if e == self.first:

                @pl.when(w >= self.slots)
                def _():
                    pl.semaphore_wait(self.s["free"].at[w - self.slots], len(self.t.everyone()))

            self.event(*e, w)
            if e == self.last:

                @pl.when(w + self.slots < MATS)
                def _():
                    for device in self.t.everyone():
                        signal(self.s["free"].at[w], device)

    def run(self):
        self.left(0, 0, 0).start()
        self.right(0, 0).start()

        def body(n, _):
            self.step(lax.div(n, self.tiles), lax.rem(n, self.tiles))
            return 0

        lax.fori_loop(0, (MATS + self.slots) * self.tiles, body, 0)


CHUNK = 256
WAVES = ((1, 1), (0, 1), (0, 3), (1, 0), (0, 0), (0, 2))
SHAPES = (UNIT, DOWN)


def tiles(R, C):
    r, c = TILE
    across, wide = C // c, UNIT[1] // c
    for n in range(R * C // (r * c)):
        yield (pl.ds(n // across * r, r), pl.ds(n % across * c, c)), (pl.ds(n // wide * r, r), pl.ds(n % wide * c, c))


def exchange_scratch():
    shapes = {}
    for kind, (R, C) in enumerate(SHAPES):
        n = sum(w[0] == kind for w in WAVES)
        shapes[f"nat{kind}"] = pltpu.VMEM((R, C), f32)
        shapes[f"slab{kind}"] = pltpu.VMEM((4, n, PADS[kind], C), bf16)
        shapes[f"rows{kind}"] = pltpu.VMEM((4, n, PADS[kind], C), bf16)
    shapes["x_send"] = pltpu.SemaphoreType.DMA((2, 4))
    shapes["x_recv"] = pltpu.SemaphoreType.DMA((2, 4))
    return shapes


def exchange(t, s):
    me = lax.rem(t.idx, 4)
    copies = []
    for o in range(1, 4):
        to = lax.rem(me + o, 4)
        for kind in range(2):
            copies.append(remote(s[f"slab{kind}"].at[to], s[f"rows{kind}"].at[me], s["x_send"].at[kind, o], s["x_recv"].at[kind, o], t.group(to)))
    for copy in copies:
        copy.start()
    for kind in range(2):
        s[f"rows{kind}"][me] = s[f"slab{kind}"][me]
    for copy in copies:
        copy.wait()


def scatter_kernel(dims, names, *refs):
    take = iter(refs)
    lefts, rights, outs = ([next(take) for _ in range(n)] for n in (MATS, MATS, 2))
    g, pg = next(take), next(take)
    s = dict(zip(names, take, strict=True))
    t = Torus(dims)
    enter(t.everyone() + [t.partner(), t.crossed()])
    sc = Scatter(dims)
    sc.bind(t, lefts, rights, g, pg, s["unit"], s)
    sc.run()
    for w, (kind, at) in enumerate(WAVES):
        R, C = SHAPES[kind]
        nat, slab = s[f"nat{kind}"], s[f"slab{kind}"]
        for natural, unit in tiles(R, C):
            nat[natural] = s["unit"][(w, *unit)]
        rows = R // 4
        for q in range(4):
            slab[q, at, 0:rows, :] = nat[q * rows : (q + 1) * rows, :].astype(bf16)
    exchange(t, s)
    for kind, out in enumerate(outs):
        C = SHAPES[kind][1]
        for q in range(4):
            out[:, :, C * q : C * (q + 1)] = s[f"rows{kind}"][q]


def places():
    return pl.BlockSpec(memory_space=pl.ANY), pl.BlockSpec(memory_space=pltpu.VMEM)


def scatter(factors, dims):
    sc = Scatter(dims)
    sc.tokens = factors[0][0].shape[0]
    scratch = sc.scratch() | {"unit": pltpu.VMEM((MATS, *UNIT), f32)} | exchange_scratch()
    anywhere, vmem = places()
    rows = [jax.ShapeDtypeStruct((sum(w[0] == kind for w in WAVES), PADS[kind], 4 * C), bf16) for kind, (_, C) in enumerate(SHAPES)]
    terms = jax.ShapeDtypeStruct((MATS, *dims, *UNIT), bf16)
    *grads, _, _ = pl.pallas_call(
        functools.partial(scatter_kernel, dims, tuple(scratch)),
        out_shape=(*rows, terms, terms),
        in_specs=[anywhere] * 2 * MATS,
        out_specs=(vmem, vmem, anywhere, anywhere),
        scratch_shapes=list(scratch.values()),
        compiler_params=pltpu.CompilerParams(collective_id=1, has_side_effects=True, vmem_limit_bytes=VMEM_MOST),
        name="scatter",
    )(*[left for left, _ in factors], *[right for _, right in factors])
    return grads


class Gather:
    def __init__(self, dims):
        self.colors = [Color(k, dims) for k in range(len(ORDERS))]
        events = [e for c in self.colors for e in c.events(True)]
        timed = []
        for n, (e, character) in enumerate(zip(events, GATHER_TIMES, strict=True)):
            for w in range(MATS):
                timed.append((time_of(character) + GATHER_STEPS[e[2] == START] * w, w, n))
        self.order = [(events[n], w) for _, w, n in sorted(timed)]

    def scratch(self):
        shapes = {}
        for c in self.colors:
            for ring in c.rings:
                for way in ("send", "recv"):
                    shapes[way + ring.name] = pltpu.SemaphoreType.DMA((MATS, ring.n - 1))
        for name in ("over_send", "over_recv"):
            shapes[name] = pltpu.SemaphoreType.DMA((MATS, len(ORDERS)))
        shapes["own"] = pltpu.SemaphoreType.DMA((MATS,))
        return shapes

    def bind(self, torus, out, unit, s):
        self.t, self.out, self.unit, self.s = torus, out, unit, s

    def place(self, c, w, core, **at):
        return self.out[w].at[(*c.index(**at), core, slice(None), c.columns)]

    def own(self, w):
        t = self.t
        return pltpu.make_async_copy(self.unit.at[w], self.out[w].at[(*t.at.values(), t.core)], self.s["own"].at[w])

    def directs(self, ring, w):
        c, t = ring.color, self.t
        src, dst = self.unit.at[w, :, c.columns], self.place(c, w, t.core, **t.at)
        return [direct(t, ring, o, w, src, dst, self.s, w, w) for o in range(1, ring.n)]

    def message(self, ring, side, m, w):
        t, c, s = self.t, ring.color, self.s
        sign = (1 - 2 * side) * (1 - 2 * (w % 2))
        at = {d: t.at[d] for d in c.order[: ring.phase]} | {ring.d: t.wrap(ring.d, t.at[ring.d] - sign * m)}
        block, n = self.place(c, w, t.core, **at), ring.message(side, m)
        return remote(block, block, s["send" + ring.name].at[w, n], s["recv" + ring.name].at[w, n], t.beside(ring.d, sign))

    def over(self, c, w, core, **at):
        block = self.place(c, w, core, **at)
        return remote(block, block, self.s["over_send"].at[w, c.k], self.s["over_recv"].at[w, c.k], self.t.partner())

    def event(self, kind, c, phase, side, j, w):
        ring, t = c.rings[phase], self.t
        if kind == "d":
            for copy in self.directs(ring, w):
                copy.start()
        elif kind == "e":
            for copy in self.directs(ring, w):
                copy.wait_recv()
        elif kind == "s":
            for side in ring.sides:
                self.message(ring, side, 0, w).start()
            if not phase:
                self.over(c, w, t.core, **{ring.d: t.at[ring.d]}).start()
        else:
            self.message(ring, side, j - 1, w).wait_recv()
            if j < ring.steps[side]:
                self.message(ring, side, j, w).start()
            if not phase:
                sign = (1 - 2 * side) * (1 - 2 * (w % 2))
                self.over(c, w, t.core, **{ring.d: t.wrap(ring.d, t.at[ring.d] - sign * j)}).start()

    def finish(self, w):
        for c in self.colors:
            for ring in c.rings:
                if ring.phase == 2:
                    for copy in self.directs(ring, w):
                        copy.wait_send()
                else:
                    for side in ring.sides:
                        for m in range(ring.steps[side]):
                            self.message(ring, side, m, w).wait_send()
            self.over(c, w, self.t.core).wait_send()
            self.over(c, w, 1 - self.t.core).wait_recv()

    def run(self):
        for w in range(MATS):
            self.own(w).wait()
        for e, w in self.order:
            self.event(*e, w)
        for w in range(MATS):
            self.finish(w)


class Exchange:
    def __init__(self, t, dims):
        X, Y, Z = dims
        near = t.cores * Z
        self.t, self.steps = t, ((near, 1, near), (X * Y, near, X * Y))

    def beside(self, n, offset):
        size, stride, _ = self.steps[n]
        idx = self.t.idx
        at = lax.rem(lax.div(idx, stride), size)
        return (self.t.rep, idx + (lax.rem(at + offset, size) - at) * stride)

    def devices(self):
        return [self.beside(n, o) for n, (size, *_) in enumerate(self.steps) for o in range(1, size)]

    def total(self, s, value):
        for n, (size, *_) in enumerate(self.steps):
            mine, box = s["norm_out"].at[n], s["norm_in"].at[n]
            mine[...] = value
            copies = [remote(mine, box.at[o], s["norm_send"].at[n, o], s["norm_recv"].at[n, o], self.beside(n, o)) for o in range(1, size)]
            for copy in copies:
                copy.start()
            for copy in copies:
                copy.wait()
            value = value + sum(box[o] for o in range(1, size))
        return value


def moments_of(g, m, v):
    return 0.9 * m + 0.1 * g, 0.95 * v + 0.05 * g * g


def rows_of(grads, kind, at):
    which, layer = (2, at) if kind else divmod(at, 2)
    return grads[kind][at, 0 : SHAPES[kind][0] // 4, :].astype(f32), which, layer


def update_kernel(dims, names, *refs):
    take = iter(refs)
    grads, w_in, m_in, v_in = ([next(take) for _ in range(n)] for n in (2, 3, 3, 3))
    factor_out, out = next(take), [next(take) for _ in WAVES]
    s = dict(zip(names, take, strict=True))
    t = Torus(dims)
    ex = Exchange(t, dims)
    enter(ex.devices())
    total, count = jnp.zeros((1, 1), f32), 0
    for kind, at in WAVES:
        g, *_ = rows_of(grads, kind, at)
        total = total + jnp.sum(jnp.sum(g * g, axis=0, keepdims=True), axis=1, keepdims=True)
        count += g.size
    for size, *_ in ex.steps:
        count *= size
    total = ex.total(s, jnp.broadcast_to(total, TILE))
    factor_out[...] = jnp.minimum(1.0, 0.5 * lax.rsqrt(total / count + 1e-30))
    factor = factor_out[0:1, 0:1]
    for kind, at in WAVES:
        g, which, layer = rows_of(grads, kind, at)
        R, C = SHAPES[kind]
        w = w_in[which][layer].astype(f32)
        m, v = moments_of(g * factor, m_in[which][:, layer, :], v_in[which][:, layer, :])
        w = (w - 0.02 * (m * lax.rsqrt(v + 1e-8) + 0.1 * w)).astype(bf16)
        for q in range(4):
            s[f"slab{kind}"][q, at, 0 : R // 4, :] = w[:, C * q : C * (q + 1)]
    exchange(t, s)
    ga = Gather(dims)
    ga.bind(t, out, s["unit"], s)
    for w, (kind, at) in enumerate(WAVES):
        R, C = SHAPES[kind]
        nat, rows_in, n = s[f"nat{kind}"], s[f"rows{kind}"], R // 4
        for q in range(4):
            nat[q * n : (q + 1) * n, :] = rows_in[q, at, 0:n, :].astype(f32)
        for natural, unit in tiles(R, C):
            s["wide"][unit] = nat[natural]
        s["unit"][w] = s["wide"][...].astype(bf16)
        ga.own(w).start()
    ga.run()


IN_VMEM = (0, 1, 2, 3)


def home(wave):
    return pltpu.VMEM if wave in IN_VMEM else pltpu.HBM


def update(grads, w, moments, dims):
    X, Y, Z = dims
    scratch = Gather(dims).scratch() | exchange_scratch()
    scratch["unit"] = pltpu.VMEM((MATS, *UNIT), bf16)
    scratch["wide"] = pltpu.VMEM(UNIT, f32)
    most = max(2 * Z, X * Y)
    scratch["norm_out"] = pltpu.VMEM((2, *TILE), f32)
    scratch["norm_in"] = pltpu.VMEM((2, most, *TILE), f32)
    for name in ("norm_send", "norm_recv"):
        scratch[name] = pltpu.SemaphoreType.DMA((2, most))
    anywhere, vmem = places()
    given = (*grads, *w, *moments)
    factor, *out = pl.pallas_call(
        functools.partial(update_kernel, dims, tuple(scratch)),
        out_shape=[jax.ShapeDtypeStruct(TILE, f32)] + [home(wave)((*dims, 2, *UNIT), bf16) for wave in range(MATS)],
        in_specs=[vmem] * len(given),
        out_specs=[vmem] + [anywhere] * MATS,
        scratch_shapes=list(scratch.values()),
        compiler_params=pltpu.CompilerParams(collective_id=2, has_side_effects=True, vmem_limit_bytes=VMEM_FEW),
        name="update",
    )(*given)
    return factor, out


VMEM_MOST, VMEM_FEW = 62 << 20, 12 << 20


def normed(h):
    wide = h.astype(f32)
    scale = lax.rsqrt(jnp.mean(wide**2, -1, keepdims=True) + 1e-6)
    return (wide * scale).astype(bf16)


def norm_back(h, da):
    wide, da = h.astype(f32), da.astype(f32)
    scale = lax.rsqrt(jnp.mean(wide**2, -1, keepdims=True) + 1e-6)
    inner = jnp.mean(wide * da, -1, keepdims=True)
    return (scale * da - wide * (inner * scale * scale * scale)).astype(bf16)


PLAIN, TURNED = ((1,), (0,)), ((1,), (1,))
ROWS = 128


def dot(a, b, dims):
    return lax.dot_general(a, b, (dims, ((), ())), preferred_element_type=f32)


def by_rows(ref, work):
    def some(i, _):
        work(pl.ds(pl.multiple_of(i * ROWS, ROWS), ROWS))
        return 0

    lax.fori_loop(0, ref.shape[0] // ROWS, some, 0)


def gate_back(dhid, gate, up):
    soft = jax.nn.sigmoid(gate)
    return dhid * up * (soft * (1.0 + gate * (1.0 - soft))), dhid * (gate * soft)


def bottom_kernel(h, wg, wu, wd, a, gate, up, hid, out, acc):
    step = pl.program_id(0)

    @pl.when(step == 0)
    def _():
        def first(rows):
            a[rows] = normed(h[rows])
            acc[rows] = jnp.zeros_like(acc[rows])

        by_rows(h, first)

    for part in parts():
        gate[:, part] = dot(a[...], wg[0, :, part], PLAIN)
        up[:, part] = dot(a[...], wu[0, :, part], PLAIN)
        hid[:, part] = (jax.nn.silu(gate[:, part]) * up[:, part]).astype(bf16)
    acc[...] += dot(hid[...], wd[0], PLAIN)

    @pl.when(step == pl.num_programs(0) - 1)
    def _():
        def last(rows):
            out[rows] = h[rows] + acc[rows].astype(bf16)

        by_rows(h, last)


def top_kernel(h, dy, wg, wu, wd, a, hid, dgate, dup, dh, acc_gate, acc_up):
    step = pl.program_id(0)

    @pl.when(step == 0)
    def _():
        def first(rows):
            a[rows] = normed(h[rows])
            for acc in (acc_gate, acc_up):
                acc[rows] = jnp.zeros_like(acc[rows])

        by_rows(h, first)

    for part in parts():
        gate = dot(a[...], wg[0, :, part], PLAIN)
        up = dot(a[...], wu[0, :, part], PLAIN)
        dhid = dot(dy[...], wd[0, part, :], TURNED).astype(bf16).astype(f32)
        hid[:, part] = (jax.nn.silu(gate) * up).astype(bf16)
        by_gate, by_up = gate_back(dhid, gate, up)
        dgate[:, part], dup[:, part] = by_gate.astype(bf16), by_up.astype(bf16)
    for acc, d, w in ((acc_gate, dgate, wg), (acc_up, dup, wu)):
        acc[...] += dot(d[...], w[0], TURNED)

    @pl.when(step == pl.num_programs(0) - 1)
    def _():
        def last(rows):
            da = acc_gate[rows].astype(bf16) + acc_up[rows].astype(bf16)
            dh[rows] = dy[rows] + norm_back(h[rows], da)

        by_rows(h, last)


def back_kernel(dh, gate, up, wd, dgate, dup):
    for part in parts():
        dhid = dot(dh[...], wd[0, part, :], TURNED).astype(bf16).astype(f32)
        by_gate, by_up = gate_back(dhid, gate[:, part], up[:, part])
        dgate[:, part], dup[:, part] = by_gate.astype(bf16), by_up.astype(bf16)


WIDTH, PART = 512, 256


def parts():
    return [slice(at, at + PART) for at in range(0, WIDTH, PART)]


def layer_call(kernel, layer, tokens_in, hidden_in, weights, hidden_out, tokens_out, accumulators, products, name):
    T, D = tokens_in[0].shape
    FF = weights[-1].shape[1]
    whole = pl.BlockSpec((T, D), lambda n: (0, 0))
    part = pl.BlockSpec((T, WIDTH), lambda n: (0, n))
    specs = [pl.BlockSpec((1, D, WIDTH), lambda n: (layer, 0, n))] * (len(weights) - 1) + [pl.BlockSpec((1, WIDTH, D), lambda n: (layer, n, 0))]
    early, late = tokens_out
    shape = jax.ShapeDtypeStruct
    return pl.pallas_call(
        kernel,
        grid=(FF // WIDTH,),
        in_specs=[whole] * len(tokens_in) + [part] * len(hidden_in) + specs,
        out_specs=[whole] * early + [part] * len(hidden_out) + [whole] * late,
        out_shape=[shape((T, D), bf16)] * early + [shape((T, FF), t) for t in hidden_out] + [shape((T, D), bf16)] * late,
        scratch_shapes=[pltpu.VMEM((T, D), f32)] * accumulators,
        cost_estimate=pl.CostEstimate(flops=2 * products * T * D * FF, bytes_accessed=2 * len(weights) * D * FF, transcendentals=T * FF),
        compiler_params=pltpu.CompilerParams(vmem_limit_bytes=VMEM_MOST),
        name=name,
    )(*tokens_in, *hidden_in, *weights)


def factors(x, dy, wg, wu, wd):
    weights = (wg, wu, wd)
    a0, gate, up, hid0, h = layer_call(bottom_kernel, 0, (x,), (), weights, (f32, f32, bf16), (1, 1), 1, 3, "bottom")
    a1, hid1, dg1, du1, dh = layer_call(top_kernel, 1, (h, dy), (), weights, (bf16,) * 3, (1, 1), 2, 5, "top")
    dg0, du0 = layer_call(back_kernel, 0, (dh,), (gate, up), (wd,), (bf16,) * 2, (0, 0), 0, 1, "back")
    return (hid1, dy), (a1, dg1), (a1, du1), (hid0, dh), (a0, dg0), (a0, du0)


SETTLED = (4, 1, 5, 2, 3, 0)
BOXES = 3


def pieces(kind):
    runs = []
    for (rows, columns), (unit_rows, unit_columns) in tiles(*SHAPES[kind]):
        if runs and runs[-1][:2] == [rows, unit_rows]:
            runs[-1][-1] += columns.size
        else:
            runs.append([rows, unit_rows, columns.start, unit_columns.start, columns.size])
    return runs


def settle_kernel(*refs):
    take = iter(refs)
    waves, grads, m_in, v_in, outs, m_out, v_out = ([next(take) for _ in range(n)] for n in (MATS, 2, 3, 3, 3, 3, 3))
    factor, box, in_sem, out_sem, near_sem = next(take), *take
    X = waves[0].shape[0]

    def put(n, x, q, block, sem):
        kind = WAVES[SETTLED[n]][0]
        C = SHAPES[kind][1]
        for rows, unit_rows, column, unit_column, width in pieces(kind):
            to = outs[n // 2].at[n % 2, x, :, :, rows, pl.ds(pl.multiple_of(C * q + column, TILE[1]), width)]
            pltpu.make_async_copy(block.at[:, :, lax.div(q, 2), lax.rem(q, 2), unit_rows, pl.ds(unit_column, width)], to, sem).start()

    def all_of(n, x, block, sem):
        lax.fori_loop(0, 4, lambda q, _: (put(n, x, q, block, sem), 0)[1], 0)

    near = [n for n, w in enumerate(SETTLED) if w in IN_VMEM]
    far = [(n, x) for n in range(MATS) if n not in near for x in range(X)]

    def fetch(k):
        n, x = far[k]
        return pltpu.make_async_copy(waves[n].at[x], box.at[k % BOXES], in_sem.at[k % BOXES])

    def drain(k):
        n, x = far[k]
        pltpu.make_async_copy(box.at[k % BOXES], waves[n].at[x], out_sem.at[k % BOXES]).wait()

    ahead = BOXES - 1
    for k in range(ahead):
        fetch(k).start()
    for n in near:
        lax.fori_loop(0, X, lambda x, _: (all_of(n, x, waves[n].at[x], near_sem.at[n]), 0)[1], 0)
    for kind, at in WAVES:
        g, which, layer = rows_of(grads, kind, at)
        m, v = moments_of(g * factor[0:1, 0:1], m_in[which][:, layer, :], v_in[which][:, layer, :])
        m_out[which][:, layer, :], v_out[which][:, layer, :] = m, v
    for k in range(len(far)):
        fetch(k).wait()
        all_of(*far[k], box.at[k % BOXES], out_sem.at[k % BOXES])
        if k + ahead < len(far):
            if k:
                drain(k - 1)
            fetch(k + ahead).start()
    for k in range(len(far) - BOXES, len(far)):
        drain(k)
    for n in near:
        pltpu.make_async_copy(waves[n], waves[n], near_sem.at[n]).wait()


def settle(waves, factor, grads, moments, dims):
    X, Y, Z = dims
    halves = Z // 2
    shape = (X, Y, halves, 2, 2, *UNIT)
    anywhere, vmem = places()
    made = jax.ShapeDtypeStruct
    R, C = zip(*SHAPES)
    outs = pl.pallas_call(
        lambda *refs: settle_kernel(*refs[: MATS + 2 + len(moments)], *refs[MATS + 3 + len(moments) : -4], refs[MATS + 2 + len(moments)], *refs[-4:]),
        out_shape=[made((2, X, Y, halves, R[which // 2], 4 * C[which // 2]), bf16) for which in range(3)] + [made(a.shape, f32) for a in moments],
        in_specs=[vmem if n in IN_VMEM else anywhere for n in SETTLED] + [vmem] * (3 + len(moments)),
        out_specs=[anywhere] * 3 + [vmem] * len(moments),
        scratch_shapes=[pltpu.VMEM((BOXES, *shape[1:]), bf16)] + [pltpu.SemaphoreType.DMA((n,)) for n in (BOXES, BOXES, MATS)],
        compiler_params=pltpu.CompilerParams(vmem_limit_bytes=VMEM_FEW),
        name="settle",
    )(*[pltpu.with_memory_space_constraint(waves[n].reshape(shape), home(n)) for n in SETTLED], *grads, *moments, factor)
    return [out.reshape(2, -1, out.shape[-1]) for out in outs[:3]], outs[3:]


def device_step(dims, x, dy, wg, wu, wd, *moments):
    grads = scatter(factors(x[0], dy[0], wg, wu, wd), dims)
    place = lax.axis_index("dp")
    w = [lax.dynamic_slice_in_dim(a, place * b.shape[1], b.shape[1], 1) for a, b in zip((wg, wu, wd), moments[:3], strict=True)]
    moments = [jnp.swapaxes(a, 0, 1) for a in moments]
    factor, waves = update(grads, w, moments, dims)
    new, moments = settle(waves, factor, grads, moments, dims)
    return (*new, *[jnp.swapaxes(a, 0, 1) for a in moments])


DIMS = {256: (4, 4, 8)}


def solution(mesh):
    dims = DIMS[mesh.shape["dp"]]
    spec = jax.sharding.PartitionSpec
    tokens, whole, rows = spec(("rep", "dp")), spec(), spec(None, "dp", None)
    return jax.shard_map(
        functools.partial(device_step, dims),
        mesh=mesh,
        in_specs=(tokens, tokens, *[whole] * 3, *[rows] * 6),
        out_specs=(*[spec("rep")] * 3, *[spec("rep", "dp", None)] * 6),
        check_vma=False,
    )
```
